128 devices in a mesh: dp: 1, ep: 128 (over z, y, x, core).
Axes of the slice: x: 4, y: 4, z: 4, core: 2. Of those that a mesh axis runs over, the one named last changes fastest.
Arguments:
- hidden: bfloat16 [65536, 768], P(('dp', 'ep'))
- logits: float32 [65536, 128], P(('dp', 'ep'))
- w_in: bfloat16 [128, 768, 3072], P('ep')
- w_out: bfloat16 [128, 3072, 768], P('ep')
Outputs:
- output: bfloat16 [65536, 768], P(('dp', 'ep'))
All inputs are finite; a program needn't handle non-finite values.
Results may differ from the reference program's by a relative error of at most 0.00468909.
Values are sent between devices in bfloat16 or wider.
A program may use at most 1 GiB of HBM per device.

```python
import jax
import jax.numpy as jnp
from jax import lax

GROUP_SIZE = 128
TOK_DEV = 512
D = 768
FF = 3072
EXPERTS = 128
CAP_FACTOR = 2

HALF_TOK = TOK_DEV // 2
TOKENS = GROUP_SIZE * TOK_DEV
MICRO_TOK = GROUP_SIZE * HALF_TOK
CAPACITY = MICRO_TOK * CAP_FACTOR // EXPERTS
PER_SRC = TOK_DEV * CAP_FACTOR // EXPERTS
OUT_GAIN = EXPERTS / (4.0 * CAP_FACTOR)


def draw_logits(route_key):
    k_src, k_split, k_pop, k_tok, k_ord = jax.random.split(route_key, 5)
    half_src = GROUP_SIZE // 2
    src_key = jax.random.randint(k_src, (2, EXPERTS, GROUP_SIZE), 0, 1 << 20) * GROUP_SIZE + jnp.arange(GROUP_SIZE)
    src_rank = jnp.argsort(jnp.argsort(src_key, axis=-1), axis=-1)
    split_amt = jax.random.randint(k_split, (2, EXPERTS, 1), 0, PER_SRC + 1)
    counts = jnp.where(src_rank < half_src - 1, PER_SRC,
                       jnp.where(src_rank == half_src - 1, split_amt,
                                 jnp.where(src_rank == half_src, PER_SRC - split_amt, 0)))
    counts = jnp.transpose(counts, (2, 0, 1))[:, :, None, :]
    popular = jax.random.randint(k_pop, (GROUP_SIZE, 2, HALF_TOK, 1), 0, 4)
    tok_noise = jax.random.randint(k_tok, (GROUP_SIZE, 2, HALF_TOK, EXPERTS), 0, 1024)
    tok_key = ((3 - popular) * 256 + tok_noise) * HALF_TOK + jnp.arange(HALF_TOK)[:, None]
    tok_rank = jnp.argsort(jnp.argsort(tok_key, axis=2), axis=2)
    chosen = (tok_rank < counts).astype(jnp.int32).reshape(TOKENS, EXPERTS)
    ord_noise = jax.random.randint(k_ord, (TOKENS, EXPERTS), 0, 256)
    col_key = (chosen * 256 + ord_noise) * TOKENS + jnp.arange(TOKENS)[:, None]
    col_rank = jnp.argsort(jnp.argsort(col_key, axis=0), axis=0)
    grid_step = (1 << 23) // TOKENS
    return (col_rank * grid_step - (TOKENS * grid_step) // 2).astype(jnp.float32) * (2.0 ** -20)


def setup_inputs(seed: int = 0, part: int = 0) -> dict:
    part_key = jax.random.fold_in(jax.random.key(seed), part)
    key_x, key_route = jax.random.split(part_key)
    key_in, key_out = jax.random.split(jax.random.key(seed + 1))
    hidden = jax.random.normal(key_x, (TOKENS, D), jnp.float32).astype(jnp.bfloat16)
    logits = draw_logits(key_route)
    w_in = (jax.random.normal(key_in, (EXPERTS, D, FF), jnp.float32) * D ** -0.5).astype(jnp.bfloat16)
    w_out = (jax.random.normal(key_out, (EXPERTS, FF, D), jnp.float32) * (OUT_GAIN * FF ** -0.5)).astype(jnp.bfloat16)
    return {"hidden": hidden, "logits": logits, "w_in": w_in, "w_out": w_out}


def reference(hidden, logits, w_in, w_out):
    gate_probs = jax.nn.softmax(logits, axis=-1)

    def by_micro(array_in):
        row_width = array_in.shape[-1]
        return array_in.reshape(GROUP_SIZE, 2, HALF_TOK, row_width).transpose(1, 0, 2, 3).reshape(2, MICRO_TOK, row_width)

    def one_micro(micro_ops):
        rows_x, rows_l, rows_g = micro_ops

        def one_expert(acc_sum, expert_ops):
            col_l, col_g, weight_a, weight_b = expert_ops
            picked = lax.top_k(col_l, CAPACITY)[1]
            pre_act = jnp.dot(rows_x[picked], weight_a, preferred_element_type=jnp.float32)
            hidden_act = jax.nn.gelu(pre_act, approximate=True).astype(jnp.bfloat16)
            expert_out = jnp.dot(hidden_act, weight_b, preferred_element_type=jnp.float32).astype(jnp.bfloat16)
            weighted = col_g[picked][:, None] * expert_out.astype(jnp.float32)
            return acc_sum.at[picked].add(weighted), None

        zero_acc = jnp.zeros((MICRO_TOK, D), jnp.float32)
        expert_sum = lax.scan(one_expert, zero_acc, (rows_l.T, rows_g.T, w_in, w_out))[0]
        return expert_sum

    micro_y = lax.map(one_micro, (by_micro(hidden), by_micro(logits), by_micro(gate_probs)))
    mixed = micro_y.reshape(2, GROUP_SIZE, HALF_TOK, D).transpose(1, 0, 2, 3).reshape(TOKENS, D)
    return (hidden.astype(jnp.float32) + mixed).astype(jnp.bfloat16)
```

```python
import functools
import math

import jax
import jax.numpy as jnp
from jax import lax
from jax.experimental import pallas as pl
from jax.experimental.pallas import tpu as pltpu
from jax.sharding import PartitionSpec as P

MESH = pl.DeviceIdType.MESH
BF16, F32 = jnp.bfloat16, jnp.float32
NDEV = 128
RANKS = 8
KEEP = 512
ORDERS = ((2, 1, 0), (1, 0, 2), (0, 2, 1))
NPART = 3
NCHUNK = 4
FSTEPS = 6


def coords(d):
    return lax.div(d, 32), lax.rem(lax.div(d, 8), 4), lax.rem(lax.div(d, 2), 4), lax.rem(d, 2)


def shifted(me, offs, core):
    pos = coords(me)
    z, y, x = (lax.rem(p + (o + 4), 4) for p, o in zip(pos[:3], offs))
    return (z * 4 + y) * 8 + x * 2 + lax.rem(pos[3] + core, 2)


def along(dim, step):
    return tuple(step if d == dim else 0 for d in range(3))


def gelu(v):
    inner = v * (0.7978845608028654 + 0.035677408136300125 * (v * v))
    half = 0.5 * v
    return half + half * jnp.tanh(inner)


def split3(v):
    a = v.astype(BF16)
    r = v - a.astype(F32)
    b = r.astype(BF16)
    c = (r - b.astype(F32)).astype(BF16)
    return a, b, c


def dot(a, b):
    return jnp.dot(a, b, preferred_element_type=F32)


def dot_t(a, b):
    return lax.dot_general(a, b, (((1,), (1,)), ((), ())), preferred_element_type=F32)


class Exchange:
    def __init__(self, me, sign, hop, mids, final, send_sem, recv_sem, cols):
        self.me, self.sign, self.hop, self.mids, self.final = me, sign, hop, mids, final
        self.send_sem, self.recv_sem, self.cols = send_sem, recv_sem, cols
        self.peers = {}
        for core in range(2):
            for dim in range(3):
                for d in range(4):
                    self.peers[dim, d, core] = shifted(me, along(dim, sign * d), core)

    def sem(self, c, p, phase):
        return (c * NPART + p) * 3 + phase

    def copy(self, src, dst, c, p, phase, d, core):
        to = self.peers[ORDERS[p][phase], d, core]
        k = self.sem(c, p, phase)
        pltpu.make_async_remote_copy(
            src, dst, self.send_sem.at[k], self.recv_sem.at[k], device_id=(0, to), device_id_type=MESH
        ).start()

    def mid_at(self, p, c, d1):
        mid = self.mids[p]
        if ORDERS[p][1] < ORDERS[p][0]:
            return mid.at[c, d1 - 1]
        return mid.at[c, :, d1 - 1]

    def final_at(self, c, p, pick):
        idx = tuple(pick[ORDERS[p].index(d)] for d in range(3))
        return self.final.at[(c, *idx, slice(None), pl.ds(p * self.cols, self.cols))]

    def send0(self, c, p):
        for d in (1, 3, 2):
            self.copy(self.hop.at[c, p, d - 1], self.hop.at[c, p, 3 + d], c, p, 0, d, 0)

    def send1(self, c, p):
        for d in (1, 3, 2):
            self.copy(self.hop.at[c, p, pl.ds(3, 4), d], self.mid_at(p, c, d), c, p, 1, d, 0)

    def send2(self, c, p):
        core = c % 2
        for d in (1, 3, 2, 0):
            if d == 0 and core == 0:
                continue
            self.copy(self.hop.at[c, p, pl.ds(3, 4), 0, d], self.final_at(c, p, (pl.ds(0, 4), 0, d)), c, p, 2, d, core)
            self.copy(self.mids[p].at[c, :, :, d], self.final_at(c, p, (pl.ds(0, 4), pl.ds(1, 3), d)), c, p, 2, d, core)

    def own(self, c, p):
        self.final_set(c, p, (pl.ds(0, 4), 0, 0), self.hop[c, p, pl.ds(3, 4), 0, 0])
        self.final_set(c, p, (pl.ds(0, 4), pl.ds(1, 3), 0), self.mids[p][c, :, :, 0])

    def final_set(self, c, p, pick, value):
        idx = tuple(pick[ORDERS[p].index(d)] for d in range(3))
        self.final[(c, *idx, slice(None), pl.ds(p * self.cols, self.cols))] = value

    def region(self, c, p, phase):
        if phase == 0:
            return self.hop.at[c, p, pl.ds(4, 3)]
        if phase == 1:
            return self.mids[p].at[c]
        part = pl.ds(0, 4) if c % 2 else pl.ds(1, 3)
        return self.final_at(c, p, (pl.ds(0, 4), pl.ds(0, 4), part))

    def wait_recv(self, c, p, phase):
        r = self.region(c, p, phase)
        pltpu.make_async_copy(r, r, self.recv_sem.at[self.sem(c, p, phase)]).wait()

    def wait_send(self, c, p, phase):
        r = self.region(c, p, phase)
        pltpu.make_async_copy(r, r, self.send_sem.at[self.sem(c, p, phase)]).wait()

    def first(self, c):
        for p in range(NPART):
            self.send0(c, p)

    def second(self, c):
        for p in range(NPART):
            self.wait_recv(c, p, 0)
            self.send1(c, p)

    def third(self, c):
        for p in range(NPART):
            self.wait_recv(c, p, 1)
            self.send2(c, p)

    def arrived(self, c):
        for p in range(NPART):
            self.wait_recv(c, p, 2)
            if c % 2 == 0:
                self.own(c, p)

    def drain(self):
        for c in range(NCHUNK):
            for p in range(NPART):
                for phase in range(3):
                    self.wait_send(c, p, phase)


def kernel(
    x_hbm, l_hbm, win_hbm, wout_hbm, out_ref,
    x_ref, l_ref, win, wout, hop_i, mid_i0, mid_i1, mid_i2, fin_i, hop_r, mid_r0, mid_r1, mid_r2, fin_r,
    place, comb, mask, tops, vsend, vrecv, rank, acc, yacc,
    load_sem, send_i, recv_i, send_r, recv_r, vsend_sem, vrecv_sem,
):
    me = lax.axis_index("ep")
    half, n_exp = l_ref.shape[0] // 2, l_ref.shape[1]
    d_model, ff = win.shape
    cols = d_model // NPART
    ftile = ff // FSTEPS
    rows = 64 * RANKS

    loads = [
        pltpu.make_async_copy(s, d, load_sem.at[i])
        for i, (s, d) in enumerate(((l_hbm, l_ref), (x_hbm, x_ref), (win_hbm.at[0], win), (wout_hbm.at[0], wout)))
    ]
    for ld in loads:
        ld.start()

    barrier = pltpu.get_barrier_semaphore()

    def hello(k, _):
        pl.semaphore_signal(barrier, inc=1, device_id=(0, lax.rem(me + k, NDEV)), device_id_type=MESH)
        return 0

    lax.fori_loop(1, NDEV, hello, 0)

    inward = Exchange(me, 1, hop_i, (mid_i0, mid_i1, mid_i2), fin_i, send_i, recv_i, cols)
    back = Exchange(me, -1, hop_r, (mid_r0, mid_r1, mid_r2), fin_r, send_r, recv_r, cols)

    pos = coords(me)
    for core in range(2):
        q = lax.broadcasted_iota(jnp.int32, (rows, n_exp), 0)
        e = lax.broadcasted_iota(jnp.int32, (rows, n_exp), 1)
        ez = ((q >> 7) + pos[0]) & 3
        ey = ((q >> 5) + pos[1]) & 3
        ex = ((q >> 3) + pos[2]) & 3
        ec = (pos[3] + core) & 1
        want = ez * 32 + ey * 8 + ex * 2 + ec
        place[core] = jnp.where(e == want, 1.0, 0.0).astype(BF16)

    def put_blocks(dst, c, value):
        for z in range(4):
            for y in range(4):
                at = (z * 4 + y) * 32
                xs = value[at : at + 32, :].reshape(4, 8, d_model).astype(BF16)
                p0, p1, p2 = (xs[:, :, p * cols : (p + 1) * cols] for p in range(NPART))
                dst[c, 0, pl.ds(0, 3), y, z] = p0[1:]
                dst[c, 0, 3, y, z] = p0[0]
                dst[c, 1, (y + 3) % 4, z] = p1
                dst[c, 2, (z + 3) % 4, :, y] = p2

    loads[0].wait()
    tops[...] = jnp.zeros_like(tops)
    for m in range(2):
        cur = l_ref[m * half : (m + 1) * half, :]
        rk = jnp.full(cur.shape, 15.0, F32)
        for r in range(RANKS):
            top = jnp.max(cur, axis=0, keepdims=True)
            hit = cur == top
            rk = jnp.where(hit, float(r), rk)
            cur = jnp.where(hit, -1e30, cur)
            tops[m * RANKS + r : m * RANKS + r + 1, :] = top
        rank[m] = rk.astype(BF16)
        if m == 0:
            loads[1].wait()
        for core in range(2):
            wide = dot_t(place[core], rank[m])
            r_of = (lax.broadcasted_iota(jnp.int32, wide.shape, 0) & 7).astype(F32)
            pick = jnp.where(wide == r_of, 1.0, 0.0).astype(BF16)
            put_blocks(hop_i, m * 2 + core, dot(pick, x_ref[m * half : (m + 1) * half, :]))
        if m == 0:
            pl.semaphore_wait(barrier, NDEV - 1)
            inward.first(0)
            inward.first(1)

    eye = jnp.where(
        lax.broadcasted_iota(jnp.int32, (n_exp, n_exp), 0) == lax.broadcasted_iota(jnp.int32, (n_exp, n_exp), 1), 1.0, 0.0
    ).astype(BF16)
    hi, mid, low = (dot_t(eye, v) for v in split3(tops[...]))
    vsend[...] = ((hi + mid) + low).reshape(n_exp, 1, n_exp)

    inward.second(0)
    inward.first(2)

    def tell(k, _):
        kz, ky, kx, kc = coords(k)
        to = shifted(me, (kz, ky, kx), kc)
        pltpu.make_async_remote_copy(
            vsend.at[to], vrecv.at[k], vsend_sem, vrecv_sem, device_id=(0, to), device_id_type=MESH
        ).start()
        return 0

    lax.fori_loop(1, NDEV, tell, 0)
    vrecv[0] = vsend[me]

    inward.second(1)

    for m in range(2):
        lg = l_ref[m * half : (m + 1) * half, :]
        ex = jnp.exp(lg - jnp.max(lg, axis=1, keepdims=True))
        terms = split3(ex / jnp.sum(ex, axis=1, keepdims=True))
        for core in range(2):
            wide = dot_t(rank[m], place[core])
            r_of = (lax.broadcasted_iota(jnp.int32, wide.shape, 1) & 7).astype(F32)
            hit = wide == r_of
            for i, term in enumerate(terms):
                comb[m * 2 + core, i] = jnp.where(hit, dot_t(term, place[core]), 0.0).astype(BF16)
        if m == 0:
            inward.third(0)
            inward.first(3)

    inward.second(2)

    told = vrecv.at[pl.ds(1, NDEV - 1)]
    pltpu.make_async_copy(told, told, vrecv_sem).wait()
    seen = vrecv[...].reshape(NDEV, n_exp)
    lane = lax.broadcasted_iota(jnp.int32, (NDEV, n_exp), 1)
    cut = None
    for m in range(2):
        mine = (lane >> 3) == m

        def bisect(_, state):
            low_end, width = state
            cand = low_end + width
            cnt = jnp.sum(jnp.where(mine & (seen >= cand), 1.0, 0.0), axis=0, keepdims=True)
            cnt = jnp.sum(cnt, axis=1, keepdims=True)
            return jnp.where(cnt >= float(KEEP), cand, low_end), width * 0.5

        t = lax.fori_loop(0, 24, bisect, (jnp.full((1, 1), -8.0, F32), jnp.full((1, 1), 8.0, F32)))[0]
        cut = t if m == 0 else jnp.where((lane >> 3) == 0, cut, t)
    chosen = jnp.where(seen >= cut, 1.0, 0.0).astype(BF16)
    for core in range(2):
        q = lax.broadcasted_iota(jnp.int32, (rows, NDEV), 0)
        src = lax.broadcasted_iota(jnp.int32, (rows, NDEV), 1)
        wide = dot(jnp.where(src == (q >> 3) * 2 + core, 1.0, 0.0).astype(BF16), chosen)
        for m in range(2):
            keep = jnp.where(src == (q & 7) + m * 8, wide, 0.0)
            mask[m * 2 + core] = jnp.sum(keep, axis=1, keepdims=True)

    inward.third(1)
    loads[2].wait()
    loads[3].wait()

    def combine(c):
        back.arrived(c)
        m, core = c // 2, c % 2
        y = fin_r[c].reshape(rows, d_model)
        total = dot(comb[c, 0], y) + dot(comb[c, 1], y) + dot(comb[c, 2], y)
        if core == 0:
            yacc[m] = total
        else:
            both = x_ref[m * half : (m + 1) * half, :].astype(F32) + (yacc[m] + total)
            out_ref[m * half : (m + 1) * half, :] = both.astype(BF16)

    during = {
        1: [lambda: inward.second(3)],
        3: [lambda: inward.third(2)],
        7: [lambda: inward.third(3)],
        12: [lambda: back.second(0)],
        15: [lambda: back.second(1)],
        17: [lambda: back.third(0)],
        19: [lambda: back.third(1)],
        21: [lambda: combine(0)],
        22: [lambda: back.second(2)],
    }

    def step(i, _):
        c, f = lax.div(i, FSTEPS), lax.rem(i, FSTEPS)
        for k in range(NCHUNK):
            @pl.when(i == k * FSTEPS)
            def _():
                inward.arrived(k)
                acc[...] = jnp.zeros_like(acc)

        at = pl.multiple_of(f * ftile, ftile)
        h = gelu(dot(fin_i[c].reshape(rows, d_model), win[:, pl.ds(at, ftile)])).astype(BF16)
        acc[...] += dot(h, wout[pl.ds(at, ftile), :])

        for k in range(NCHUNK):
            @pl.when(i == k * FSTEPS + FSTEPS - 1)
            def _():
                put_blocks(hop_r, k, jnp.where(mask[k] > 0.5, acc[...], 0.0))
                back.first(k)
        for at_i, todo in during.items():
            @pl.when(i == at_i)
            def _():
                for fn in todo:
                    fn()
        return 0

    lax.fori_loop(0, NCHUNK * FSTEPS, step, 0)

    combine(1)
    back.third(2)
    back.second(3)
    combine(2)
    back.third(3)
    combine(3)

    inward.drain()
    back.drain()
    sent = vsend.at[pl.ds(1, NDEV - 1)]
    pltpu.make_async_copy(sent, sent, vsend_sem).wait()


def layer(hidden, logits, w_in, w_out):
    tok, d_model = hidden.shape
    n_exp = logits.shape[1]
    ff = w_in.shape[2]
    cols = d_model // NPART
    half = tok // 2

    def path():
        mids = [
            pltpu.VMEM((NCHUNK, *((3, 4) if o[1] < o[0] else (4, 3)), 4, RANKS, cols), BF16) for o in ORDERS
        ]
        return [pltpu.VMEM((NCHUNK, NPART, 7, 4, 4, RANKS, cols), BF16), *mids, pltpu.VMEM((NCHUNK, 4, 4, 4, RANKS, d_model), BF16)]

    n_sem = NCHUNK * NPART * 3
    dma = pltpu.SemaphoreType.DMA
    return pl.pallas_call(
        kernel,
        out_shape=jax.ShapeDtypeStruct(hidden.shape, hidden.dtype),
        in_specs=[pl.BlockSpec(memory_space=pl.ANY)] * 4,
        out_specs=pl.BlockSpec(memory_space=pltpu.VMEM),
        scratch_shapes=[
            pltpu.VMEM((tok, d_model), BF16),
            pltpu.VMEM((tok, n_exp), F32),
            pltpu.VMEM((d_model, ff), BF16),
            pltpu.VMEM((ff, d_model), BF16),
            *path(),
            *path(),
            pltpu.VMEM((2, 512, n_exp), BF16),
            pltpu.VMEM((NCHUNK, 3, half, 512), BF16),
            pltpu.VMEM((NCHUNK, 512, 1), F32),
            pltpu.VMEM((n_exp, n_exp), F32),
            pltpu.VMEM((NDEV, 1, n_exp), F32),
            pltpu.VMEM((NDEV, 1, n_exp), F32),
            pltpu.VMEM((2, half, n_exp), BF16),
            pltpu.VMEM((512, d_model), F32),
            pltpu.VMEM((2, half, d_model), F32),
            dma((4,)),
            dma((n_sem,)),
            dma((n_sem,)),
            dma((n_sem,)),
            dma((n_sem,)),
            dma,
            dma,
        ],
        compiler_params=pltpu.CompilerParams(collective_id=0, has_side_effects=True, vmem_limit_bytes=60 << 20),
    )(hidden, logits, w_in, w_out)


def solution(mesh):
    tok = P(("dp", "ep"), None)
    exp = P("ep", None, None)
    return jax.shard_map(layer, mesh=mesh, in_specs=(tok, tok, exp, exp), out_specs=tok, check_vma=False)
```

```python
import functools
import math

import jax
import jax.numpy as jnp
from jax import lax
from jax.experimental import pallas as pl
from jax.experimental.pallas import tpu as pltpu
from jax.sharding import PartitionSpec as P

MESH = pl.DeviceIdType.MESH
BF16, F32 = jnp.bfloat16, jnp.float32
NDEV = 128
RANKS = 8
KEEP = 512
ORDERS = ((2, 1, 0), (1, 0, 2), (0, 2, 1))
NPART = 3
NCHUNK = 4
FSTEPS = 6


def coords(d):
    return lax.div(d, 32), lax.rem(lax.div(d, 8), 4), lax.rem(lax.div(d, 2), 4), lax.rem(d, 2)


def shifted(me, offs, core):
    pos = coords(me)
    z, y, x = (lax.rem(p + (o + 4), 4) for p, o in zip(pos[:3], offs))
    return (z * 4 + y) * 8 + x * 2 + lax.rem(pos[3] + core, 2)


def along(dim, step):
    return tuple(step if d == dim else 0 for d in range(3))


def gelu(v):
    inner = v * (0.7978845608028654 + 0.035677408136300125 * (v * v))
    half = 0.5 * v
    return half + half * jnp.tanh(inner)


def split3(v):
    a = v.astype(BF16)
    r = v - a.astype(F32)
    b = r.astype(BF16)
    c = (r - b.astype(F32)).astype(BF16)
    return a, b, c


def dot(a, b):
    return jnp.dot(a, b, preferred_element_type=F32)


def dot_t(a, b):
    return lax.dot_general(a, b, (((1,), (1,)), ((), ())), preferred_element_type=F32)


class Exchange:
    def __init__(self, me, sign, hop, mids, final, send_sem, recv_sem, cols):
        self.me, self.sign, self.hop, self.mids, self.final = me, sign, hop, mids, final
        self.send_sem, self.recv_sem, self.cols = send_sem, recv_sem, cols
        self.peers = {}
        for core in range(2):
            for dim in range(3):
                for d in range(4):
                    self.peers[dim, d, core] = shifted(me, along(dim, sign * d), core)

    def sem(self, c, p, phase):
        return (c * NPART + p) * 3 + phase

    def copy(self, src, dst, c, p, phase, d, core):
        to = self.peers[ORDERS[p][phase], d, core]
        k = self.sem(c, p, phase)
        pltpu.make_async_remote_copy(
            src, dst, self.send_sem.at[k], self.recv_sem.at[k], device_id=(0, to), device_id_type=MESH
        ).start()

    def mid_at(self, p, c, d1):
        mid = self.mids[p]
        if ORDERS[p][1] < ORDERS[p][0]:
            return mid.at[c, d1 - 1]
        return mid.at[c, :, d1 - 1]

    def final_at(self, c, p, pick):
        idx = tuple(pick[ORDERS[p].index(d)] for d in range(3))
        return self.final.at[(c, *idx, slice(None), pl.ds(p * self.cols, self.cols))]

    def send0(self, c, p):
        for d in (1, 3, 2):
            self.copy(self.hop.at[c, p, d - 1], self.hop.at[c, p, 3 + d], c, p, 0, d, 0)

    def send1(self, c, p):
        for d in (1, 3, 2):
            self.copy(self.hop.at[c, p, pl.ds(3, 4), d], self.mid_at(p, c, d), c, p, 1, d, 0)

    def send2(self, c, p):
        core = c % 2
        for d in (1, 3, 2, 0):
            if d == 0 and core == 0:
                continue
            self.copy(self.hop.at[c, p, pl.ds(3, 4), 0, d], self.final_at(c, p, (pl.ds(0, 4), 0, d)), c, p, 2, d, core)
            self.copy(self.mids[p].at[c, :, :, d], self.final_at(c, p, (pl.ds(0, 4), pl.ds(1, 3), d)), c, p, 2, d, core)

    def own(self, c, p):
        self.final_set(c, p, (pl.ds(0, 4), 0, 0), self.hop[c, p, pl.ds(3, 4), 0, 0])
        self.final_set(c, p, (pl.ds(0, 4), pl.ds(1, 3), 0), self.mids[p][c, :, :, 0])

    def final_set(self, c, p, pick, value):
        idx = tuple(pick[ORDERS[p].index(d)] for d in range(3))
        self.final[(c, *idx, slice(None), pl.ds(p * self.cols, self.cols))] = value

    def region(self, c, p, phase):
        if phase == 0:
            return self.hop.at[c, p, pl.ds(4, 3)]
        if phase == 1:
            return self.mids[p].at[c]
        part = pl.ds(0, 4) if c % 2 else pl.ds(1, 3)
        return self.final_at(c, p, (pl.ds(0, 4), pl.ds(0, 4), part))

    def wait_recv(self, c, p, phase):
        r = self.region(c, p, phase)
        pltpu.make_async_copy(r, r, self.recv_sem.at[self.sem(c, p, phase)]).wait()

    def wait_send(self, c, p, phase):
        r = self.region(c, p, phase)
        pltpu.make_async_copy(r, r, self.send_sem.at[self.sem(c, p, phase)]).wait()

    def first(self, c):
        for p in range(NPART):
            self.send0(c, p)

    def second(self, c):
        for p in range(NPART):
            self.wait_recv(c, p, 0)
            self.send1(c, p)

    def third(self, c):
        for p in range(NPART):
            self.wait_recv(c, p, 1)
            self.send2(c, p)

    def arrived_part(self, c, p):
        self.wait_recv(c, p, 2)
        if c % 2 == 0:
            self.own(c, p)

    def arrived(self, c):
        for p in range(NPART):
            self.arrived_part(c, p)

    def drain(self):
        for c in range(NCHUNK):
            for p in range(NPART):
                for phase in range(3):
                    self.wait_send(c, p, phase)


def kernel(
    x_hbm, l_hbm, win_hbm, wout_hbm, out_ref,
    x_ref, l_ref, win, wout, hop_i, mid_i0, mid_i1, mid_i2, fin_i, hop_r, mid_r0, mid_r1, mid_r2, fin_r,
    place, comb, mask, tops, tell_hop, tell_mid, told, rank, acc, yacc,
    load_sem, send_i, recv_i, send_r, recv_r, tell_send, tell_recv,
):
    me = lax.axis_index("ep")
    half, n_exp = l_ref.shape[0] // 2, l_ref.shape[1]
    d_model, ff = win.shape
    cols = d_model // NPART
    ftile = ff // FSTEPS
    rows = 64 * RANKS

    loads = [
        pltpu.make_async_copy(s, d, load_sem.at[i])
        for i, (s, d) in enumerate(((l_hbm, l_ref), (x_hbm, x_ref), (win_hbm.at[0], win), (wout_hbm.at[0], wout)))
    ]
    for ld in loads:
        ld.start()

    barrier = pltpu.get_barrier_semaphore()

    inward = Exchange(me, 1, hop_i, (mid_i0, mid_i1, mid_i2), fin_i, send_i, recv_i, cols)
    back = Exchange(me, -1, hop_r, (mid_r0, mid_r1, mid_r2), fin_r, send_r, recv_r, cols)

    peers = [inward.peers[dim, d, core] for core in range(2) for dim in range(3) for d in (1, 2, 3)] + [inward.peers[0, 0, 1]]
    for to in peers:
        pl.semaphore_signal(barrier, inc=1, device_id=(0, to), device_id_type=MESH)

    pos = coords(me)
    for core in range(2):
        q = lax.broadcasted_iota(jnp.int32, (rows, n_exp), 0)
        e = lax.broadcasted_iota(jnp.int32, (rows, n_exp), 1)
        ez = ((q >> 7) + pos[0]) & 3
        ey = ((q >> 5) + pos[1]) & 3
        ex = ((q >> 3) + pos[2]) & 3
        ec = (pos[3] + core) & 1
        want = ez * 32 + ey * 8 + ex * 2 + ec
        place[core] = jnp.where(e == want, 1.0, 0.0).astype(BF16)

    def put_blocks(dst, c, value):
        for z in range(4):
            for y in range(4):
                at = (z * 4 + y) * 32
                xs = value[at : at + 32, :].reshape(4, 8, d_model).astype(BF16)
                p0, p1, p2 = (xs[:, :, p * cols : (p + 1) * cols] for p in range(NPART))
                dst[c, 0, pl.ds(0, 3), y, z] = p0[1:]
                dst[c, 0, 3, y, z] = p0[0]
                dst[c, 1, (y + 3) % 4, z] = p1
                dst[c, 2, (z + 3) % 4, :, y] = p2

    def select(m):
        cur = l_ref[m * half : (m + 1) * half, :]
        rk = jnp.full(cur.shape, 15.0, F32)
        for r in range(RANKS):
            top = jnp.max(cur, axis=0, keepdims=True)
            hit = cur == top
            rk = jnp.where(hit, float(r), rk)
            cur = jnp.where(hit, -1e30, cur)
            for g in range(8):
                at = g * 16 + m * RANKS + r
                tops[at : at + 1, :] = top
        rank[m] = rk.astype(BF16)

    def gather(c):
        m, core = c // 2, c % 2
        wide = dot_t(place[core], rank[m])
        r_of = (lax.broadcasted_iota(jnp.int32, wide.shape, 0) & 7).astype(F32)
        pick = jnp.where(wide == r_of, 1.0, 0.0).astype(BF16)
        put_blocks(hop_i, c, dot(pick, x_ref[m * half : (m + 1) * half, :]))

    def tell_copy(src, dst, phase, dim, d, core):
        pltpu.make_async_remote_copy(
            src, dst, tell_send.at[phase], tell_recv.at[phase], device_id=(0, inward.peers[dim, d, core]), device_id_type=MESH
        ).start()

    def tell_wait(sem, phase, ref):
        pltpu.make_async_copy(ref, ref, sem.at[phase]).wait()

    def tell_first():
        q = lax.broadcasted_iota(jnp.int32, (NDEV, n_exp), 0)
        e = lax.broadcasted_iota(jnp.int32, (NDEV, n_exp), 1)
        ex = ((q >> 5) + 1 + pos[2]) & 3
        ey = ((q >> 3) + pos[1]) & 3
        ez = ((q >> 1) + pos[0]) & 3
        ec = (q + pos[3]) & 1
        at = jnp.where(e == ez * 32 + ey * 8 + ex * 2 + ec, 1.0, 0.0).astype(BF16)
        hi, mid, low = (dot_t(at, v) for v in split3(tops[...]))
        tell_hop[0:4] = ((hi + mid) + low).reshape(4, 4, 4, 2, 1, n_exp)
        for d in (1, 3, 2):
            tell_copy(tell_hop.at[d - 1], tell_hop.at[3 + d], 0, 2, d, 0)

    def tell_second():
        tell_wait(tell_recv, 0, tell_hop.at[pl.ds(4, 3)])
        for d in (1, 3, 2):
            tell_copy(tell_hop.at[pl.ds(3, 4), d], tell_mid.at[d - 1], 1, 1, d, 0)

    def tell_third():
        tell_wait(tell_recv, 1, tell_mid)
        for core in range(2):
            for d in (1, 3, 2, 0):
                if core or d:
                    tell_copy(tell_hop.at[pl.ds(3, 4), 0, d, core], told.at[core, d, 0], 3 - core, 0, d, core)
                    tell_copy(tell_mid.at[:, :, d, core], told.at[core, d, pl.ds(1, 3)], 3 - core, 0, d, core)

    def owner_cut():
        for ref, sem in ((told.at[1], tell_recv.at[2]), (told.at[0, pl.ds(1, 3)], tell_recv.at[3])):
            pltpu.make_async_copy(ref, ref, sem).wait()
        told[0, 0, 0] = tell_hop[3:7, 0, 0, 0]
        told[0, 0, 1:4] = tell_mid[:, :, 0, 0]
        seen = told[...].reshape(NDEV, n_exp)
        lane = lax.broadcasted_iota(jnp.int32, (n_exp, n_exp), 1)
        row = lax.broadcasted_iota(jnp.int32, (n_exp, n_exp), 0)
        same = jnp.where((lane >> 3) == (row >> 3), 1.0, 0.0).astype(BF16)
        first = jnp.where(((row & 7) == 0) & (((lane >> 3) & 1) == ((row >> 3) & 1)), 1.0, 0.0).astype(BF16)
        group = (lax.broadcasted_iota(jnp.int32, (8, n_exp), 1) >> 4).astype(F32)
        base = jnp.full((8, n_exp), -8.0, F32)
        width = 2.0
        for _ in range(8):
            cand = base + group * width
            over = jnp.where(seen >= cand[0:1], 1.0, 0.0)
            cnt = jnp.sum(over, axis=0, keepdims=True)
            cnt = dot(jnp.broadcast_to(cnt, (8, n_exp)).astype(BF16), same)
            flag = jnp.where(cnt >= float(KEEP), 1.0, 0.0).astype(BF16)
            base = base + (dot(flag, first) - 1.0) * width
            width = width / 8.0
        chosen = jnp.where(seen >= base[0:1], 1.0, 0.0).astype(BF16)
        for core in range(2):
            q = lax.broadcasted_iota(jnp.int32, (rows, NDEV), 0)
            src = lax.broadcasted_iota(jnp.int32, (rows, NDEV), 1)
            wide = dot(jnp.where(src == (q >> 3) + core * 64, 1.0, 0.0).astype(BF16), chosen)
            for m in range(2):
                keep = jnp.where(src == (q & 7) + m * 8, wide, 0.0)
                mask[m * 2 + core] = jnp.sum(keep, axis=1, keepdims=True)

    def gates():
        for m in range(2):
            lg = l_ref[m * half : (m + 1) * half, :]
            ex = jnp.exp(lg - jnp.max(lg, axis=1, keepdims=True))
            terms = split3(ex / jnp.sum(ex, axis=1, keepdims=True))
            for core in range(2):
                wide = dot_t(rank[m], place[core])
                r_of = (lax.broadcasted_iota(jnp.int32, wide.shape, 1) & 7).astype(F32)
                hit = wide == r_of
                for i, term in enumerate(terms):
                    comb[m * 2 + core, i] = jnp.where(hit, dot_t(term, place[core]), 0.0).astype(BF16)

    def combine(c):
        m, core = c // 2, c % 2
        for p in range(NPART):
            back.arrived_part(c, p)
            at = slice(p * cols, (p + 1) * cols)
            y = fin_r[c, :, :, :, :, at].reshape(rows, cols)
            total = dot(comb[c, 0], y) + dot(comb[c, 1], y) + dot(comb[c, 2], y)
            if core == 0:
                yacc[m, :, at] = total
            else:
                both = x_ref[m * half : (m + 1) * half, at].astype(F32) + (yacc[m, :, at] + total)
                out_ref[m * half : (m + 1) * half, at] = both.astype(BF16)

    loads[0].wait()
    tops[...] = jnp.zeros_like(tops)
    select(0)
    loads[1].wait()
    gather(0)
    pl.semaphore_wait(barrier, len(peers))
    inward.first(0)
    gather(1)
    inward.first(1)
    select(1)
    tell_first()
    gather(2)
    gather(3)
    inward.first(3)
    gates()
    inward.second(0)
    tell_second()
    inward.first(2)
    inward.second(1)
    tell_third()
    inward.third(0)
    owner_cut()
    inward.second(2)
    inward.third(1)
    loads[2].wait()
    loads[3].wait()

    during = {
        1: [lambda: inward.second(3)],
        3: [lambda: inward.third(2)],
        7: [lambda: inward.third(3)],
        14: [lambda: back.second(0)],
        18: [lambda: back.second(1)],
    }

    def step(i, _):
        c, f = lax.div(i, FSTEPS), lax.rem(i, FSTEPS)
        for k in range(NCHUNK):
            @pl.when(i == k * FSTEPS)
            def _():
                inward.arrived(k)
                acc[...] = jnp.zeros_like(acc)

        at = pl.multiple_of(f * ftile, ftile)
        h = gelu(dot(fin_i[c].reshape(rows, d_model), win[:, pl.ds(at, ftile)])).astype(BF16)
        acc[...] += dot(h, wout[pl.ds(at, ftile), :])

        for k in range(NCHUNK):
            @pl.when(i == k * FSTEPS + FSTEPS - 1)
            def _():
                put_blocks(hop_r, k, jnp.where(mask[k] > 0.5, acc[...], 0.0))
                back.first(k)
        for at_i, todo in during.items():
            @pl.when(i == at_i)
            def _():
                for fn in todo:
                    fn()
        return 0

    lax.fori_loop(0, NCHUNK * FSTEPS, step, 0)

    back.second(2)
    back.third(0)
    back.second(3)
    back.third(2)
    back.third(1)
    back.third(3)
    combine(0)
    combine(1)
    combine(2)
    combine(3)

    inward.drain()
    back.drain()
    tell_wait(tell_send, 0, tell_hop.at[pl.ds(4, 3)])
    tell_wait(tell_send, 1, tell_mid)
    for ref, sem in ((told.at[1], tell_send.at[2]), (told.at[0, pl.ds(1, 3)], tell_send.at[3])):
        pltpu.make_async_copy(ref, ref, sem).wait()


def layer(hidden, logits, w_in, w_out):
    tok, d_model = hidden.shape
    n_exp = logits.shape[1]
    ff = w_in.shape[2]
    cols = d_model // NPART
    half = tok // 2

    def path():
        mids = [
            pltpu.VMEM((NCHUNK, *((3, 4) if o[1] < o[0] else (4, 3)), 4, RANKS, cols), BF16) for o in ORDERS
        ]
        return [pltpu.VMEM((NCHUNK, NPART, 7, 4, 4, RANKS, cols), BF16), *mids, pltpu.VMEM((NCHUNK, 4, 4, 4, RANKS, d_model), BF16)]

    n_sem = NCHUNK * NPART * 3
    dma = pltpu.SemaphoreType.DMA
    return pl.pallas_call(
        kernel,
        out_shape=jax.ShapeDtypeStruct(hidden.shape, hidden.dtype),
        in_specs=[pl.BlockSpec(memory_space=pl.ANY)] * 4,
        out_specs=pl.BlockSpec(memory_space=pltpu.VMEM),
        scratch_shapes=[
            pltpu.VMEM((tok, d_model), BF16),
            pltpu.VMEM((tok, n_exp), F32),
            pltpu.VMEM((d_model, ff), BF16),
            pltpu.VMEM((ff, d_model), BF16),
            *path(),
            *path(),
            pltpu.VMEM((2, 512, n_exp), BF16),
            pltpu.VMEM((NCHUNK, 3, half, 512), BF16),
            pltpu.VMEM((NCHUNK, 512, 1), F32),
            pltpu.VMEM((n_exp, n_exp), F32),
            pltpu.VMEM((7, 4, 4, 2, 1, n_exp), F32),
            pltpu.VMEM((3, 4, 4, 2, 1, n_exp), F32),
            pltpu.VMEM((2, 4, 4, 4, 1, n_exp), F32),
            pltpu.VMEM((2, half, n_exp), BF16),
            pltpu.VMEM((512, d_model), F32),
            pltpu.VMEM((2, half, d_model), F32),
            dma((4,)),
            dma((n_sem,)),
            dma((n_sem,)),
            dma((n_sem,)),
            dma((n_sem,)),
            dma((4,)),
            dma((4,)),
        ],
        compiler_params=pltpu.CompilerParams(collective_id=0, has_side_effects=True, vmem_limit_bytes=60 << 20),
    )(hidden, logits, w_in, w_out)


def solution(mesh):
    tok = P(("dp", "ep"), None)
    exp = P("ep", None, None)
    return jax.shard_map(layer, mesh=mesh, in_specs=(tok, tok, exp, exp), out_specs=tok, check_vma=False)
```

```python
import functools
import math

import jax
import jax.numpy as jnp
from jax import lax
from jax.experimental import pallas as pl
from jax.experimental.pallas import tpu as pltpu
from jax.sharding import PartitionSpec as P

MESH = pl.DeviceIdType.MESH
BF16, F32 = jnp.bfloat16, jnp.float32
NDEV = 128
RANKS = 8
KEEP = 512
ORDERS = ((2, 1, 0), (1, 0, 2), (0, 2, 1))
NPART = 3
NCHUNK = 4
FSTEPS = 6


def coords(d):
    return lax.div(d, 32), lax.rem(lax.div(d, 8), 4), lax.rem(lax.div(d, 2), 4), lax.rem(d, 2)


def shifted(me, offs, core):
    pos = coords(me)
    z, y, x = (lax.rem(p + (o + 4), 4) for p, o in zip(pos[:3], offs))
    return (z * 4 + y) * 8 + x * 2 + lax.rem(pos[3] + core, 2)


def along(dim, step):
    return tuple(step if d == dim else 0 for d in range(3))


def gelu(v):
    inner = v * (0.7978845608028654 + 0.035677408136300125 * (v * v))
    half = 0.5 * v
    return half + half * jnp.tanh(inner)


def split3(v):
    a = v.astype(BF16)
    r = v - a.astype(F32)
    b = r.astype(BF16)
    c = (r - b.astype(F32)).astype(BF16)
    return a, b, c


def dot(a, b):
    return jnp.dot(a, b, preferred_element_type=F32)


def dot_t(a, b):
    return lax.dot_general(a, b, (((1,), (1,)), ((), ())), preferred_element_type=F32)


class Exchange:
    def __init__(self, me, sign, hop, mids, final, send_sem, recv_sem, cols):
        self.me, self.sign, self.hop, self.mids, self.final = me, sign, hop, mids, final
        self.send_sem, self.recv_sem, self.cols = send_sem, recv_sem, cols
        self.peers = {}
        for core in range(2):
            for dim in range(3):
                for d in range(4):
                    self.peers[dim, d, core] = shifted(me, along(dim, sign * d), core)

    def sem(self, c, p, phase):
        return (c * NPART + p) * 3 + phase

    def copy(self, src, dst, c, p, phase, d, core):
        to = self.peers[ORDERS[p][phase], d, core]
        k = self.sem(c, p, phase)
        pltpu.make_async_remote_copy(
            src, dst, self.send_sem.at[k], self.recv_sem.at[k], device_id=(0, to), device_id_type=MESH
        ).start()

    def mid_at(self, p, c, d1):
        mid = self.mids[p]
        if ORDERS[p][1] < ORDERS[p][0]:
            return mid.at[c, d1 - 1]
        return mid.at[c, :, d1 - 1]

    def final_at(self, c, p, pick):
        idx = tuple(pick[ORDERS[p].index(d)] for d in range(3))
        return self.final.at[(c, *idx, slice(None), pl.ds(p * self.cols, self.cols))]

    def send0(self, c, p):
        for d in (1, 3, 2):
            self.copy(self.hop.at[c, p, d - 1], self.hop.at[c, p, 3 + d], c, p, 0, d, 0)

    def send1(self, c, p):
        for d in (1, 3, 2):
            self.copy(self.hop.at[c, p, pl.ds(3, 4), d], self.mid_at(p, c, d), c, p, 1, d, 0)

    def send2(self, c, p):
        core = c % 2
        for d in (1, 3, 2, 0):
            if d == 0 and core == 0:
                continue
            self.copy(self.hop.at[c, p, pl.ds(3, 4), 0, d], self.final_at(c, p, (pl.ds(0, 4), 0, d)), c, p, 2, d, core)
            self.copy(self.mids[p].at[c, :, :, d], self.final_at(c, p, (pl.ds(0, 4), pl.ds(1, 3), d)), c, p, 2, d, core)

    def own(self, c, p):
        self.final_set(c, p, (pl.ds(0, 4), 0, 0), self.hop[c, p, pl.ds(3, 4), 0, 0])
        self.final_set(c, p, (pl.ds(0, 4), pl.ds(1, 3), 0), self.mids[p][c, :, :, 0])

    def final_set(self, c, p, pick, value):
        idx = tuple(pick[ORDERS[p].index(d)] for d in range(3))
        self.final[(c, *idx, slice(None), pl.ds(p * self.cols, self.cols))] = value

    def region(self, c, p, phase):
        if phase == 0:
            return self.hop.at[c, p, pl.ds(4, 3)]
        if phase == 1:
            return self.mids[p].at[c]
        part = pl.ds(0, 4) if c % 2 else pl.ds(1, 3)
        return self.final_at(c, p, (pl.ds(0, 4), pl.ds(0, 4), part))

    def wait_recv(self, c, p, phase):
        r = self.region(c, p, phase)
        pltpu.make_async_copy(r, r, self.recv_sem.at[self.sem(c, p, phase)]).wait()

    def wait_send(self, c, p, phase):
        r = self.region(c, p, phase)
        pltpu.make_async_copy(r, r, self.send_sem.at[self.sem(c, p, phase)]).wait()

    def first(self, c):
        for p in range(NPART):
            self.send0(c, p)

    def second(self, c):
        for p in range(NPART):
            self.wait_recv(c, p, 0)
            self.send1(c, p)

    def third(self, c):
        for p in range(NPART):
            self.wait_recv(c, p, 1)
            self.send2(c, p)

    def arrived_part(self, c, p):
        self.wait_recv(c, p, 2)
        if c % 2 == 0:
            self.own(c, p)

    def arrived(self, c):
        for p in range(NPART):
            self.arrived_part(c, p)

    def drain(self):
        for c in range(NCHUNK):
            for p in range(NPART):
                for phase in range(3):
                    self.wait_send(c, p, phase)


def kernel(
    x_hbm, l_hbm, win_hbm, wout_hbm, out_ref,
    x_ref, l_ref, win, wout, hop_i, mid_i0, mid_i1, mid_i2, fin_i, hop_r, mid_r0, mid_r1, mid_r2, fin_r,
    place, comb, mask, tops, tell_hop, tell_mid, told, rank, acc, yacc,
    load_sem, send_i, recv_i, send_r, recv_r, tell_send, tell_recv,
):
    me = lax.axis_index("ep")
    half, n_exp = l_ref.shape[0] // 2, l_ref.shape[1]
    d_model, ff = win.shape
    cols = d_model // NPART
    ftile = ff // FSTEPS
    rows = 64 * RANKS

    loads = [
        pltpu.make_async_copy(s, d, load_sem.at[i])
        for i, (s, d) in enumerate(((l_hbm, l_ref), (x_hbm, x_ref), (win_hbm.at[0], win), (wout_hbm.at[0], wout)))
    ]
    for ld in loads:
        ld.start()

    barrier = pltpu.get_barrier_semaphore()

    inward = Exchange(me, 1, hop_i, (mid_i0, mid_i1, mid_i2), fin_i, send_i, recv_i, cols)
    back = Exchange(me, -1, hop_r, (mid_r0, mid_r1, mid_r2), fin_r, send_r, recv_r, cols)

    peers = [inward.peers[dim, d, core] for core in range(2) for dim in range(3) for d in (1, 2, 3)] + [inward.peers[0, 0, 1]]
    for to in peers:
        pl.semaphore_signal(barrier, inc=1, device_id=(0, to), device_id_type=MESH)

    pos = coords(me)
    for core in range(2):
        q = lax.broadcasted_iota(jnp.int32, (rows, n_exp), 0)
        e = lax.broadcasted_iota(jnp.int32, (rows, n_exp), 1)
        ez = ((q >> 7) + pos[0]) & 3
        ey = ((q >> 5) + pos[1]) & 3
        ex = ((q >> 3) + pos[2]) & 3
        ec = (pos[3] + core) & 1
        want = ez * 32 + ey * 8 + ex * 2 + ec
        place[core] = jnp.where(e == want, 1.0, 0.0).astype(BF16)

    def put_blocks(dst, c, value):
        for z in range(4):
            for y in range(4):
                at = (z * 4 + y) * 32
                xs = value[at : at + 32, :].reshape(4, 8, d_model).astype(BF16)
                p0, p1, p2 = (xs[:, :, p * cols : (p + 1) * cols] for p in range(NPART))
                dst[c, 0, pl.ds(0, 3), y, z] = p0[1:]
                dst[c, 0, 3, y, z] = p0[0]
                dst[c, 1, (y + 3) % 4, z] = p1
                dst[c, 2, (z + 3) % 4, :, y] = p2

    def select(m):
        cur = l_ref[m * half : (m + 1) * half, :]
        rk = jnp.full(cur.shape, 15.0, F32)
        for r in range(RANKS):
            top = jnp.max(cur, axis=0, keepdims=True)
            hit = cur == top
            rk = jnp.where(hit, float(r), rk)
            cur = jnp.where(hit, -1e30, cur)
            for g in range(8):
                at = g * 16 + m * RANKS + r
                tops[at : at + 1, :] = top
        rank[m] = rk.astype(BF16)

    def gather(c):
        m, core = c // 2, c % 2
        wide = dot_t(place[core], rank[m])
        r_of = (lax.broadcasted_iota(jnp.int32, wide.shape, 0) & 7).astype(F32)
        pick = jnp.where(wide == r_of, 1.0, 0.0).astype(BF16)
        put_blocks(hop_i, c, dot(pick, x_ref[m * half : (m + 1) * half, :]))

    def tell_copy(src, dst, phase, dim, d, core):
        pltpu.make_async_remote_copy(
            src, dst, tell_send.at[phase], tell_recv.at[phase], device_id=(0, inward.peers[dim, d, core]), device_id_type=MESH
        ).start()

    def tell_wait(sem, phase, ref):
        pltpu.make_async_copy(ref, ref, sem.at[phase]).wait()

    def tell_first():
        q = lax.broadcasted_iota(jnp.int32, (NDEV, n_exp), 0)
        e = lax.broadcasted_iota(jnp.int32, (NDEV, n_exp), 1)
        ex = ((q >> 5) + 1 + pos[2]) & 3
        ey = ((q >> 3) + pos[1]) & 3
        ez = ((q >> 1) + pos[0]) & 3
        ec = (q + pos[3]) & 1
        at = jnp.where(e == ez * 32 + ey * 8 + ex * 2 + ec, 1.0, 0.0).astype(BF16)
        hi, mid, low = (dot_t(at, v) for v in split3(tops[...]))
        tell_hop[0:4] = ((hi + mid) + low).reshape(4, 4, 4, 2, 1, n_exp)
        for d in (1, 3, 2):
            tell_copy(tell_hop.at[d - 1], tell_hop.at[3 + d], 0, 2, d, 0)

    def tell_second():
        tell_wait(tell_recv, 0, tell_hop.at[pl.ds(4, 3)])
        for d in (1, 3, 2):
            tell_copy(tell_hop.at[pl.ds(3, 4), d], tell_mid.at[d - 1], 1, 1, d, 0)

    def tell_third():
        tell_wait(tell_recv, 1, tell_mid)
        for core in range(2):
            for d in (1, 3, 2, 0):
                if core or d:
                    tell_copy(tell_hop.at[pl.ds(3, 4), 0, d, core], told.at[core, d, 0], 3 - core, 0, d, core)
                    tell_copy(tell_mid.at[:, :, d, core], told.at[core, d, pl.ds(1, 3)], 3 - core, 0, d, core)

    def owner_cut():
        for ref, sem in ((told.at[1], tell_recv.at[2]), (told.at[0, pl.ds(1, 3)], tell_recv.at[3])):
            pltpu.make_async_copy(ref, ref, sem).wait()
        told[0, 0, 0] = tell_hop[3:7, 0, 0, 0]
        told[0, 0, 1:4] = tell_mid[:, :, 0, 0]
        seen = told[...].reshape(NDEV, n_exp)
        lane = lax.broadcasted_iota(jnp.int32, (n_exp, n_exp), 1)
        row = lax.broadcasted_iota(jnp.int32, (n_exp, n_exp), 0)
        same = jnp.where((lane >> 3) == (row >> 3), 1.0, 0.0).astype(BF16)
        first = jnp.where(((row & 7) == 0) & (((lane >> 3) & 1) == ((row >> 3) & 1)), 1.0, 0.0).astype(BF16)
        group = (lax.broadcasted_iota(jnp.int32, (8, n_exp), 1) >> 4).astype(F32)
        base = jnp.full((8, n_exp), -8.0, F32)
        width = 2.0
        for _ in range(8):
            cand = base + group * width
            over = jnp.where(seen >= cand[0:1], 1.0, 0.0)
            cnt = jnp.sum(over, axis=0, keepdims=True)
            cnt = dot(jnp.broadcast_to(cnt, (8, n_exp)).astype(BF16), same)
            flag = jnp.where(cnt >= float(KEEP), 1.0, 0.0).astype(BF16)
            base = base + (dot(flag, first) - 1.0) * width
            width = width / 8.0
        chosen = jnp.where(seen >= base[0:1], 1.0, 0.0).astype(BF16)
        for core in range(2):
            q = lax.broadcasted_iota(jnp.int32, (rows, NDEV), 0)
            src = lax.broadcasted_iota(jnp.int32, (rows, NDEV), 1)
            wide = dot(jnp.where(src == (q >> 3) + core * 64, 1.0, 0.0).astype(BF16), chosen)
            for m in range(2):
                keep = jnp.where(src == (q & 7) + m * 8, wide, 0.0)
                mask[m * 2 + core] = jnp.sum(keep, axis=1, keepdims=True)

    def gates():
        for m in range(2):
            lg = l_ref[m * half : (m + 1) * half, :]
            ex = jnp.exp(lg - jnp.max(lg, axis=1, keepdims=True))
            terms = split3(ex / jnp.sum(ex, axis=1, keepdims=True))
            for core in range(2):
                wide = dot_t(rank[m], place[core])
                r_of = (lax.broadcasted_iota(jnp.int32, wide.shape, 1) & 7).astype(F32)
                hit = wide == r_of
                for i, term in enumerate(terms):
                    comb[m * 2 + core, i] = jnp.where(hit, dot_t(term, place[core]), 0.0).astype(BF16)

    def combine(c):
        m, core = c // 2, c % 2
        for p in range(NPART):
            back.arrived_part(c, p)
            at = slice(p * cols, (p + 1) * cols)
            y = fin_r[c, :, :, :, :, at].reshape(rows, cols)
            total = dot(comb[c, 0], y) + dot(comb[c, 1], y) + dot(comb[c, 2], y)
            if core == 0:
                yacc[m, :, at] = total
            else:
                both = x_ref[m * half : (m + 1) * half, at].astype(F32) + (yacc[m, :, at] + total)
                out_ref[m * half : (m + 1) * half, at] = both.astype(BF16)

    def more():
        gather(2)
        gather(3)

    loads[0].wait()
    tops[...] = jnp.zeros_like(tops)
    select(0)
    loads[1].wait()
    gather(0)
    pl.semaphore_wait(barrier, len(peers))
    inward.first(0)
    select(1)
    tell_first()
    gather(1)
    inward.first(1)
    inward.second(0)
    inward.second(1)
    more()
    tell_second()
    inward.third(0)
    inward.first(2)
    tell_third()
    inward.first(3)
    inward.third(1)
    loads[2].wait()
    loads[3].wait()

    during = {
        2: [lambda: inward.second(2), lambda: owner_cut()],
        4: [lambda: inward.second(3)],
        7: [lambda: inward.third(2)],
        11: [lambda: inward.third(3)],
        12: [lambda: back.second(0)],
        15: [lambda: back.second(1)],
        18: [lambda: back.third(0)],
        20: [lambda: back.third(1)],
    }

    def step(i, _):
        c, f = lax.div(i, FSTEPS), lax.rem(i, FSTEPS)
        for k in range(NCHUNK):
            @pl.when(i == k * FSTEPS)
            def _():
                inward.arrived(k)
                acc[...] = jnp.zeros_like(acc)

        at = pl.multiple_of(f * ftile, ftile)
        h = gelu(dot(fin_i[c].reshape(rows, d_model), win[:, pl.ds(at, ftile)])).astype(BF16)
        acc[...] += dot(h, wout[pl.ds(at, ftile), :])

        for k in range(NCHUNK):
            @pl.when(i == k * FSTEPS + FSTEPS - 1)
            def _():
                put_blocks(hop_r, k, jnp.where(mask[k] > 0.5, acc[...], 0.0))
                back.first(k)
        for at_i, todo in during.items():
            @pl.when(i == at_i)
            def _():
                for fn in todo:
                    fn()
        return 0

    lax.fori_loop(0, NCHUNK * FSTEPS, step, 0)

    back.second(2)
    back.second(3)
    gates()
    back.third(2)
    back.third(3)
    combine(0)
    combine(1)
    combine(2)
    combine(3)

    inward.drain()
    back.drain()
    tell_wait(tell_send, 0, tell_hop.at[pl.ds(4, 3)])
    tell_wait(tell_send, 1, tell_mid)
    for ref, sem in ((told.at[1], tell_send.at[2]), (told.at[0, pl.ds(1, 3)], tell_send.at[3])):
        pltpu.make_async_copy(ref, ref, sem).wait()


def layer(hidden, logits, w_in, w_out):
    tok, d_model = hidden.shape
    n_exp = logits.shape[1]
    ff = w_in.shape[2]
    cols = d_model // NPART
    half = tok // 2

    def path():
        mids = [
            pltpu.VMEM((NCHUNK, *((3, 4) if o[1] < o[0] else (4, 3)), 4, RANKS, cols), BF16) for o in ORDERS
        ]
        return [pltpu.VMEM((NCHUNK, NPART, 7, 4, 4, RANKS, cols), BF16), *mids, pltpu.VMEM((NCHUNK, 4, 4, 4, RANKS, d_model), BF16)]

    n_sem = NCHUNK * NPART * 3
    dma = pltpu.SemaphoreType.DMA
    return pl.pallas_call(
        kernel,
        out_shape=jax.ShapeDtypeStruct(hidden.shape, hidden.dtype),
        in_specs=[pl.BlockSpec(memory_space=pl.ANY)] * 4,
        out_specs=pl.BlockSpec(memory_space=pltpu.VMEM),
        scratch_shapes=[
            pltpu.VMEM((tok, d_model), BF16),
            pltpu.VMEM((tok, n_exp), F32),
            pltpu.VMEM((d_model, ff), BF16),
            pltpu.VMEM((ff, d_model), BF16),
            *path(),
            *path(),
            pltpu.VMEM((2, 512, n_exp), BF16),
            pltpu.VMEM((NCHUNK, 3, half, 512), BF16),
            pltpu.VMEM((NCHUNK, 512, 1), F32),
            pltpu.VMEM((n_exp, n_exp), F32),
            pltpu.VMEM((7, 4, 4, 2, 1, n_exp), F32),
            pltpu.VMEM((3, 4, 4, 2, 1, n_exp), F32),
            pltpu.VMEM((2, 4, 4, 4, 1, n_exp), F32),
            pltpu.VMEM((2, half, n_exp), BF16),
            pltpu.VMEM((512, d_model), F32),
            pltpu.VMEM((2, half, d_model), F32),
            dma((4,)),
            dma((n_sem,)),
            dma((n_sem,)),
            dma((n_sem,)),
            dma((n_sem,)),
            dma((4,)),
            dma((4,)),
        ],
        compiler_params=pltpu.CompilerParams(collective_id=0, has_side_effects=True, vmem_limit_bytes=60 << 20),
    )(hidden, logits, w_in, w_out)


def solution(mesh):
    tok = P(("dp", "ep"), None)
    exp = P("ep", None, None)
    return jax.shard_map(layer, mesh=mesh, in_specs=(tok, tok, exp, exp), out_specs=tok, check_vma=False)
```

```python
import functools
import math

import jax
import jax.numpy as jnp
from jax import lax
from jax.experimental import pallas as pl
from jax.experimental.pallas import tpu as pltpu
from jax.sharding import PartitionSpec as P

MESH = pl.DeviceIdType.MESH
BF16, F32 = jnp.bfloat16, jnp.float32
NDEV = 128
RANKS = 8
KEEP = 512
ORDERS = ((2, 1, 0), (1, 0, 2), (0, 2, 1))
NPART = 3
NCHUNK = 4
FSTEPS = 6


def coords(d):
    return lax.div(d, 32), lax.rem(lax.div(d, 8), 4), lax.rem(lax.div(d, 2), 4), lax.rem(d, 2)


def shifted(me, offs, core):
    pos = coords(me)
    z, y, x = (lax.rem(p + (o + 4), 4) for p, o in zip(pos[:3], offs))
    return (z * 4 + y) * 8 + x * 2 + lax.rem(pos[3] + core, 2)


def along(dim, step):
    return tuple(step if d == dim else 0 for d in range(3))


def gelu(v):
    inner = v * (0.7978845608028654 + 0.035677408136300125 * (v * v))
    half = 0.5 * v
    return half + half * jnp.tanh(inner)


def split3(v):
    a = v.astype(BF16)
    r = v - a.astype(F32)
    b = r.astype(BF16)
    c = (r - b.astype(F32)).astype(BF16)
    return a, b, c


def dot(a, b):
    return jnp.dot(a, b, preferred_element_type=F32)


def dot_t(a, b):
    return lax.dot_general(a, b, (((1,), (1,)), ((), ())), preferred_element_type=F32)


class Exchange:
    def __init__(self, me, sign, hop, mids, final, send_sem, recv_sem, cols):
        self.me, self.sign, self.hop, self.mids, self.final = me, sign, hop, mids, final
        self.send_sem, self.recv_sem, self.cols = send_sem, recv_sem, cols
        self.peers = {}
        for core in range(2):
            for dim in range(3):
                for d in range(4):
                    self.peers[dim, d, core] = shifted(me, along(dim, sign * d), core)

    def sem(self, c, p, phase):
        return (c * NPART + p) * 3 + phase

    def copy(self, src, dst, c, p, phase, d, core):
        to = self.peers[ORDERS[p][phase], d, core]
        k = self.sem(c, p, phase)
        pltpu.make_async_remote_copy(
            src, dst, self.send_sem.at[k], self.recv_sem.at[k], device_id=(0, to), device_id_type=MESH
        ).start()

    def mid_at(self, p, c, d1):
        mid = self.mids[p]
        if ORDERS[p][1] < ORDERS[p][0]:
            return mid.at[c, d1 - 1]
        return mid.at[c, :, d1 - 1]

    def final_at(self, c, p, pick):
        idx = tuple(pick[ORDERS[p].index(d)] for d in range(3))
        return self.final.at[(c, *idx, slice(None), pl.ds(p * self.cols, self.cols))]

    def send0(self, c, p):
        for d in (1, 3, 2):
            self.copy(self.hop.at[c, p, d - 1], self.hop.at[c, p, 3 + d], c, p, 0, d, 0)

    def send1(self, c, p):
        for d in (1, 3, 2):
            self.copy(self.hop.at[c, p, pl.ds(3, 4), d], self.mid_at(p, c, d), c, p, 1, d, 0)

    def send2(self, c, p):
        core = c % 2
        for d in (1, 3, 2, 0):
            if d == 0 and core == 0:
                continue
            self.copy(self.hop.at[c, p, pl.ds(3, 4), 0, d], self.final_at(c, p, (pl.ds(0, 4), 0, d)), c, p, 2, d, core)
            self.copy(self.mids[p].at[c, :, :, d], self.final_at(c, p, (pl.ds(0, 4), pl.ds(1, 3), d)), c, p, 2, d, core)

    def own(self, c, p):
        self.final_set(c, p, (pl.ds(0, 4), 0, 0), self.hop[c, p, pl.ds(3, 4), 0, 0])
        self.final_set(c, p, (pl.ds(0, 4), pl.ds(1, 3), 0), self.mids[p][c, :, :, 0])

    def final_set(self, c, p, pick, value):
        idx = tuple(pick[ORDERS[p].index(d)] for d in range(3))
        self.final[(c, *idx, slice(None), pl.ds(p * self.cols, self.cols))] = value

    def region(self, c, p, phase):
        if phase == 0:
            return self.hop.at[c, p, pl.ds(4, 3)]
        if phase == 1:
            return self.mids[p].at[c]
        part = pl.ds(0, 4) if c % 2 else pl.ds(1, 3)
        return self.final_at(c, p, (pl.ds(0, 4), pl.ds(0, 4), part))

    def wait_recv(self, c, p, phase):
        r = self.region(c, p, phase)
        pltpu.make_async_copy(r, r, self.recv_sem.at[self.sem(c, p, phase)]).wait()

    def wait_send(self, c, p, phase):
        r = self.region(c, p, phase)
        pltpu.make_async_copy(r, r, self.send_sem.at[self.sem(c, p, phase)]).wait()

    def first(self, c):
        for p in range(NPART):
            self.send0(c, p)

    def second(self, c):
        for p in range(NPART):
            self.wait_recv(c, p, 0)
            self.send1(c, p)

    def third(self, c):
        for p in range(NPART):
            self.wait_recv(c, p, 1)
            self.send2(c, p)

    def arrived_part(self, c, p):
        self.wait_recv(c, p, 2)
        if c % 2 == 0:
            self.own(c, p)

    def arrived(self, c):
        for p in range(NPART):
            self.arrived_part(c, p)

    def drain(self):
        for c in range(NCHUNK):
            for p in range(NPART):
                for phase in range(3):
                    self.wait_send(c, p, phase)


def kernel(
    x_ref, l_ref, win_hbm, wout_hbm, out_ref,
    win, wout, hop_i, mid_i0, mid_i1, mid_i2, fin_i, hop_r, mid_r0, mid_r1, mid_r2, fin_r,
    place, comb, mask, tops, tell_hop, tell_mid, told, rank, acc, yacc,
    load_sem, send_i, recv_i, send_r, recv_r, tell_send, tell_recv,
):
    me = lax.axis_index("ep")
    half, n_exp = l_ref.shape[0] // 2, l_ref.shape[1]
    d_model, ff = win.shape
    cols = d_model // NPART
    ftile = ff // FSTEPS
    rows = 64 * RANKS

    loads = [
        pltpu.make_async_copy(s, d, load_sem.at[i])
        for i, (s, d) in enumerate(((win_hbm.at[0], win), (wout_hbm.at[0], wout)))
    ]
    for ld in loads:
        ld.start()

    barrier = pltpu.get_barrier_semaphore()

    inward = Exchange(me, 1, hop_i, (mid_i0, mid_i1, mid_i2), fin_i, send_i, recv_i, cols)
    back = Exchange(me, -1, hop_r, (mid_r0, mid_r1, mid_r2), fin_r, send_r, recv_r, cols)

    peers = [inward.peers[dim, d, core] for core in range(2) for dim in range(3) for d in (1, 2, 3)] + [inward.peers[0, 0, 1]]
    for to in peers:
        pl.semaphore_signal(barrier, inc=1, device_id=(0, to), device_id_type=MESH)

    pos = coords(me)
    for core in range(2):
        q = lax.broadcasted_iota(jnp.int32, (rows, n_exp), 0)
        e = lax.broadcasted_iota(jnp.int32, (rows, n_exp), 1)
        ez = ((q >> 7) + pos[0]) & 3
        ey = ((q >> 5) + pos[1]) & 3
        ex = ((q >> 3) + pos[2]) & 3
        ec = (pos[3] + core) & 1
        want = ez * 32 + ey * 8 + ex * 2 + ec
        place[core] = jnp.where(e == want, 1.0, 0.0).astype(BF16)

    def put_blocks(dst, c, value):
        for z in range(4):
            for y in range(4):
                at = (z * 4 + y) * 32
                xs = value[at : at + 32, :].reshape(4, 8, d_model).astype(BF16)
                p0, p1, p2 = (xs[:, :, p * cols : (p + 1) * cols] for p in range(NPART))
                dst[c, 0, pl.ds(0, 3), y, z] = p0[1:]
                dst[c, 0, 3, y, z] = p0[0]
                dst[c, 1, (y + 3) % 4, z] = p1
                dst[c, 2, (z + 3) % 4, :, y] = p2

    def select(m):
        cur = l_ref[m * half : (m + 1) * half, :]
        rk = jnp.full(cur.shape, 15.0, F32)
        for r in range(RANKS):
            top = jnp.max(cur, axis=0, keepdims=True)
            hit = cur == top
            rk = jnp.where(hit, float(r), rk)
            cur = jnp.where(hit, -1e30, cur)
            for g in range(8):
                at = g * 16 + m * RANKS + r
                tops[at : at + 1, :] = top
        rank[m] = rk.astype(BF16)

    def gather(c):
        m, core = c // 2, c % 2
        wide = dot_t(place[core], rank[m])
        r_of = (lax.broadcasted_iota(jnp.int32, wide.shape, 0) & 7).astype(F32)
        pick = jnp.where(wide == r_of, 1.0, 0.0).astype(BF16)
        put_blocks(hop_i, c, dot(pick, x_ref[m * half : (m + 1) * half, :]))

    def tell_copy(src, dst, phase, dim, d, core):
        pltpu.make_async_remote_copy(
            src, dst, tell_send.at[phase], tell_recv.at[phase], device_id=(0, inward.peers[dim, d, core]), device_id_type=MESH
        ).start()

    def tell_wait(sem, phase, ref):
        pltpu.make_async_copy(ref, ref, sem.at[phase]).wait()

    def tell_first():
        q = lax.broadcasted_iota(jnp.int32, (NDEV, n_exp), 0)
        e = lax.broadcasted_iota(jnp.int32, (NDEV, n_exp), 1)
        ex = ((q >> 5) + 1 + pos[2]) & 3
        ey = ((q >> 3) + pos[1]) & 3
        ez = ((q >> 1) + pos[0]) & 3
        ec = (q + pos[3]) & 1
        at = jnp.where(e == ez * 32 + ey * 8 + ex * 2 + ec, 1.0, 0.0).astype(BF16)
        hi, mid, low = (dot_t(at, v) for v in split3(tops[...]))
        tell_hop[0:4] = ((hi + mid) + low).reshape(4, 4, 4, 2, 1, n_exp)
        for d in (1, 3, 2):
            tell_copy(tell_hop.at[d - 1], tell_hop.at[3 + d], 0, 2, d, 0)

    def tell_second():
        tell_wait(tell_recv, 0, tell_hop.at[pl.ds(4, 3)])
        for d in (1, 3, 2):
            tell_copy(tell_hop.at[pl.ds(3, 4), d], tell_mid.at[d - 1], 1, 1, d, 0)

    def tell_third():
        tell_wait(tell_recv, 1, tell_mid)
        for core in range(2):
            for d in (1, 3, 2, 0):
                if core or d:
                    tell_copy(tell_hop.at[pl.ds(3, 4), 0, d, core], told.at[core, d, 0], 3 - core, 0, d, core)
                    tell_copy(tell_mid.at[:, :, d, core], told.at[core, d, pl.ds(1, 3)], 3 - core, 0, d, core)

    def owner_cut():
        for ref, sem in ((told.at[1], tell_recv.at[2]), (told.at[0, pl.ds(1, 3)], tell_recv.at[3])):
            pltpu.make_async_copy(ref, ref, sem).wait()
        told[0, 0, 0] = tell_hop[3:7, 0, 0, 0]
        told[0, 0, 1:4] = tell_mid[:, :, 0, 0]
        seen = told[...].reshape(NDEV, n_exp)
        lane = lax.broadcasted_iota(jnp.int32, (n_exp, n_exp), 1)
        row = lax.broadcasted_iota(jnp.int32, (n_exp, n_exp), 0)
        same = jnp.where((lane >> 3) == (row >> 3), 1.0, 0.0).astype(BF16)
        first = jnp.where(((row & 7) == 0) & (((lane >> 3) & 1) == ((row >> 3) & 1)), 1.0, 0.0).astype(BF16)
        group = (lax.broadcasted_iota(jnp.int32, (8, n_exp), 1) >> 4).astype(F32)
        base = jnp.full((8, n_exp), -8.0, F32)
        width = 2.0
        for _ in range(8):
            cand = base + group * width
            over = jnp.where(seen >= cand[0:1], 1.0, 0.0)
            cnt = jnp.sum(over, axis=0, keepdims=True)
            cnt = dot(jnp.broadcast_to(cnt, (8, n_exp)).astype(BF16), same)
            flag = jnp.where(cnt >= float(KEEP), 1.0, 0.0).astype(BF16)
            base = base + (dot(flag, first) - 1.0) * width
            width = width / 8.0
        chosen = jnp.where(seen >= base[0:1], 1.0, 0.0).astype(BF16)
        for core in range(2):
            q = lax.broadcasted_iota(jnp.int32, (rows, NDEV), 0)
            src = lax.broadcasted_iota(jnp.int32, (rows, NDEV), 1)
            wide = dot(jnp.where(src == (q >> 3) + core * 64, 1.0, 0.0).astype(BF16), chosen)
            for m in range(2):
                keep = jnp.where(src == (q & 7) + m * 8, wide, 0.0)
                mask[m * 2 + core] = jnp.sum(keep, axis=1, keepdims=True)

    def gates():
        for m in range(2):
            lg = l_ref[m * half : (m + 1) * half, :]
            ex = jnp.exp(lg - jnp.max(lg, axis=1, keepdims=True))
            terms = split3(ex / jnp.sum(ex, axis=1, keepdims=True))
            for core in range(2):
                wide = dot_t(rank[m], place[core])
                r_of = (lax.broadcasted_iota(jnp.int32, wide.shape, 1) & 7).astype(F32)
                hit = wide == r_of
                for i, term in enumerate(terms):
                    comb[m * 2 + core, i] = jnp.where(hit, dot_t(term, place[core]), 0.0).astype(BF16)

    def combine(c):
        m, core = c // 2, c % 2
        for p in range(NPART):
            back.arrived_part(c, p)
            at = slice(p * cols, (p + 1) * cols)
            y = fin_r[c, :, :, :, :, at].reshape(rows, cols)
            total = dot(comb[c, 0], y) + dot(comb[c, 1], y) + dot(comb[c, 2], y)
            if core == 0:
                yacc[m, :, at] = total
            else:
                both = x_ref[m * half : (m + 1) * half, at].astype(F32) + (yacc[m, :, at] + total)
                out_ref[m * half : (m + 1) * half, at] = both.astype(BF16)

    def more():
        gather(2)
        gather(3)

    tops[...] = jnp.zeros_like(tops)
    select(0)
    gather(0)
    pl.semaphore_wait(barrier, len(peers))
    inward.first(0)
    select(1)
    tell_first()
    gather(1)
    inward.first(1)
    inward.second(0)
    inward.second(1)
    more()
    tell_second()
    inward.third(0)
    inward.first(2)
    tell_third()
    inward.first(3)
    inward.third(1)
    loads[0].wait()
    loads[1].wait()

    during = {
        2: [lambda: inward.second(2), lambda: owner_cut()],
        4: [lambda: inward.second(3)],
        7: [lambda: inward.third(2)],
        11: [lambda: inward.third(3)],
        12: [lambda: back.second(0)],
        15: [lambda: back.second(1)],
        18: [lambda: back.third(0)],
        20: [lambda: back.third(1)],
    }

    def step(i, _):
        c, f = lax.div(i, FSTEPS), lax.rem(i, FSTEPS)
        for k in range(NCHUNK):
            @pl.when(i == k * FSTEPS)
            def _():
                inward.arrived(k)
                acc[...] = jnp.zeros_like(acc)

        at = pl.multiple_of(f * ftile, ftile)
        h = gelu(dot(fin_i[c].reshape(rows, d_model), win[:, pl.ds(at, ftile)])).astype(BF16)
        acc[...] += dot(h, wout[pl.ds(at, ftile), :])

        for k in range(NCHUNK):
            @pl.when(i == k * FSTEPS + FSTEPS - 1)
            def _():
                put_blocks(hop_r, k, jnp.where(mask[k] > 0.5, acc[...], 0.0))
                back.first(k)
        for at_i, todo in during.items():
            @pl.when(i == at_i)
            def _():
                for fn in todo:
                    fn()
        return 0

    lax.fori_loop(0, NCHUNK * FSTEPS, step, 0)

    back.second(2)
    back.second(3)
    gates()
    back.third(2)
    back.third(3)
    combine(0)
    combine(1)
    combine(2)
    combine(3)

    inward.drain()
    back.drain()
    tell_wait(tell_send, 0, tell_hop.at[pl.ds(4, 3)])
    tell_wait(tell_send, 1, tell_mid)
    for ref, sem in ((told.at[1], tell_send.at[2]), (told.at[0, pl.ds(1, 3)], tell_send.at[3])):
        pltpu.make_async_copy(ref, ref, sem).wait()


def layer(hidden, logits, w_in, w_out):
    tok, d_model = hidden.shape
    n_exp = logits.shape[1]
    ff = w_in.shape[2]
    cols = d_model // NPART
    half = tok // 2

    def path():
        mids = [
            pltpu.VMEM((NCHUNK, *((3, 4) if o[1] < o[0] else (4, 3)), 4, RANKS, cols), BF16) for o in ORDERS
        ]
        return [pltpu.VMEM((NCHUNK, NPART, 7, 4, 4, RANKS, cols), BF16), *mids, pltpu.VMEM((NCHUNK, 4, 4, 4, RANKS, d_model), BF16)]

    n_sem = NCHUNK * NPART * 3
    dma = pltpu.SemaphoreType.DMA
    return pl.pallas_call(
        kernel,
        out_shape=jax.ShapeDtypeStruct(hidden.shape, hidden.dtype),
        in_specs=[pl.BlockSpec(memory_space=pltpu.VMEM)] * 2 + [pl.BlockSpec(memory_space=pl.ANY)] * 2,
        out_specs=pl.BlockSpec(memory_space=pltpu.VMEM),
        scratch_shapes=[
            pltpu.VMEM((d_model, ff), BF16),
            pltpu.VMEM((ff, d_model), BF16),
            *path(),
            *path(),
            pltpu.VMEM((2, 512, n_exp), BF16),
            pltpu.VMEM((NCHUNK, 3, half, 512), BF16),
            pltpu.VMEM((NCHUNK, 512, 1), F32),
            pltpu.VMEM((n_exp, n_exp), F32),
            pltpu.VMEM((7, 4, 4, 2, 1, n_exp), F32),
            pltpu.VMEM((3, 4, 4, 2, 1, n_exp), F32),
            pltpu.VMEM((2, 4, 4, 4, 1, n_exp), F32),
            pltpu.VMEM((2, half, n_exp), BF16),
            pltpu.VMEM((512, d_model), F32),
            pltpu.VMEM((2, half, d_model), F32),
            dma((2,)),
            dma((n_sem,)),
            dma((n_sem,)),
            dma((n_sem,)),
            dma((n_sem,)),
            dma((4,)),
            dma((4,)),
        ],
        compiler_params=pltpu.CompilerParams(collective_id=0, has_side_effects=True, vmem_limit_bytes=52 << 20),
    )(hidden, logits, w_in, w_out)


def solution(mesh):
    tok = P(("dp", "ep"), None)
    exp = P("ep", None, None)
    return jax.shard_map(layer, mesh=mesh, in_specs=(tok, tok, exp, exp), out_specs=tok, check_vma=False)
```

```python
import functools
import math

import jax
import jax.numpy as jnp
from jax import lax
from jax.experimental import pallas as pl
from jax.experimental.pallas import tpu as pltpu
from jax.sharding import PartitionSpec as P

MESH = pl.DeviceIdType.MESH
BF16, F32 = jnp.bfloat16, jnp.float32
NDEV = 128
RANKS = 8
KEEP = 512
ORDERS = ((2, 1, 0), (1, 0, 2), (0, 2, 1))
NPART = 3
NCHUNK = 4
FSTEPS = 6


def coords(d):
    return lax.div(d, 32), lax.rem(lax.div(d, 8), 4), lax.rem(lax.div(d, 2), 4), lax.rem(d, 2)


def shifted(me, offs, core):
    pos = coords(me)
    z, y, x = (lax.rem(p + (o + 4), 4) for p, o in zip(pos[:3], offs))
    return (z * 4 + y) * 8 + x * 2 + lax.rem(pos[3] + core, 2)


def along(dim, step):
    return tuple(step if d == dim else 0 for d in range(3))


def gelu(v):
    inner = v * (0.7978845608028654 + 0.035677408136300125 * (v * v))
    half = 0.5 * v
    return half + half * jnp.tanh(inner)


def split3(v):
    a = v.astype(BF16)
    r = v - a.astype(F32)
    b = r.astype(BF16)
    c = (r - b.astype(F32)).astype(BF16)
    return a, b, c


def dot(a, b):
    return jnp.dot(a, b, preferred_element_type=F32)


def dot_t(a, b):
    return lax.dot_general(a, b, (((1,), (1,)), ((), ())), preferred_element_type=F32)


class Exchange:
    def __init__(self, me, sign, hop, mids, final, send_sem, recv_sem, cols):
        self.me, self.sign, self.hop, self.mids, self.final = me, sign, hop, mids, final
        self.send_sem, self.recv_sem, self.cols = send_sem, recv_sem, cols
        self.peers = {}
        for core in range(2):
            for dim in range(3):
                for d in range(4):
                    self.peers[dim, d, core] = shifted(me, along(dim, sign * d), core)

    def sem(self, c, p, phase):
        return (c * NPART + p) * 3 + phase

    def copy(self, src, dst, c, p, phase, d, core):
        to = self.peers[ORDERS[p][phase], d, core]
        k = self.sem(c, p, phase)
        pltpu.make_async_remote_copy(
            src, dst, self.send_sem.at[k], self.recv_sem.at[k], device_id=(0, to), device_id_type=MESH
        ).start()

    def mid_at(self, p, c, d1):
        mid = self.mids[p]
        if ORDERS[p][1] < ORDERS[p][0]:
            return mid.at[c, d1 - 1]
        return mid.at[c, :, d1 - 1]

    def final_at(self, c, p, pick):
        idx = tuple(pick[ORDERS[p].index(d)] for d in range(3))
        return self.final.at[(c, *idx, slice(None), pl.ds(p * self.cols, self.cols))]

    def send0(self, c, p):
        for d in (1, 3, 2):
            self.copy(self.hop.at[c, p, d - 1], self.hop.at[c, p, 3 + d], c, p, 0, d, 0)

    def send1(self, c, p):
        for d in (1, 3, 2):
            self.copy(self.hop.at[c, p, pl.ds(3, 4), d], self.mid_at(p, c, d), c, p, 1, d, 0)

    def send2(self, c, p):
        core = c % 2
        for d in (1, 3, 2, 0):
            if d == 0 and core == 0:
                continue
            self.copy(self.hop.at[c, p, pl.ds(3, 4), 0, d], self.final_at(c, p, (pl.ds(0, 4), 0, d)), c, p, 2, d, core)
            self.copy(self.mids[p].at[c, :, :, d], self.final_at(c, p, (pl.ds(0, 4), pl.ds(1, 3), d)), c, p, 2, d, core)

    def own(self, c, p):
        self.final_set(c, p, (pl.ds(0, 4), 0, 0), self.hop[c, p, pl.ds(3, 4), 0, 0])
        self.final_set(c, p, (pl.ds(0, 4), pl.ds(1, 3), 0), self.mids[p][c, :, :, 0])

    def final_set(self, c, p, pick, value):
        idx = tuple(pick[ORDERS[p].index(d)] for d in range(3))
        self.final[(c, *idx, slice(None), pl.ds(p * self.cols, self.cols))] = value

    def region(self, c, p, phase):
        if phase == 0:
            return self.hop.at[c, p, pl.ds(4, 3)]
        if phase == 1:
            return self.mids[p].at[c]
        part = pl.ds(0, 4) if c % 2 else pl.ds(1, 3)
        return self.final_at(c, p, (pl.ds(0, 4), pl.ds(0, 4), part))

    def wait_recv(self, c, p, phase):
        r = self.region(c, p, phase)
        pltpu.make_async_copy(r, r, self.recv_sem.at[self.sem(c, p, phase)]).wait()

    def wait_send(self, c, p, phase):
        r = self.region(c, p, phase)
        pltpu.make_async_copy(r, r, self.send_sem.at[self.sem(c, p, phase)]).wait()

    def first(self, c):
        for p in range(NPART):
            self.send0(c, p)

    def second(self, c):
        for p in range(NPART):
            self.wait_recv(c, p, 0)
            self.send1(c, p)

    def third(self, c):
        for p in range(NPART):
            self.wait_recv(c, p, 1)
            self.send2(c, p)

    def arrived_part(self, c, p):
        self.wait_recv(c, p, 2)
        if c % 2 == 0:
            self.own(c, p)

    def arrived(self, c):
        for p in range(NPART):
            self.arrived_part(c, p)

    def drain(self):
        for c in range(NCHUNK):
            for p in range(NPART):
                for phase in range(3):
                    self.wait_send(c, p, phase)


def kernel(
    x_hbm, l_hbm, win_hbm, wout_hbm, out_ref,
    x_ref, l_ref, win, wout, hop_i, mid_i0, mid_i1, mid_i2, fin_i, hop_r, mid_r0, mid_r1, mid_r2, fin_r,
    place, comb, mask, tops, tell_hop, tell_mid, told, rank, acc, yacc,
    load_sem, send_i, recv_i, send_r, recv_r, tell_send, tell_recv,
):
    me = lax.axis_index("ep")
    half, n_exp = l_ref.shape[0] // 2, l_ref.shape[1]
    d_model, ff = win.shape
    cols = d_model // NPART
    ftile = ff // FSTEPS
    rows = 64 * RANKS

    loads = [
        pltpu.make_async_copy(s, d, load_sem.at[i])
        for i, (s, d) in enumerate(((l_hbm, l_ref), (x_hbm, x_ref), (win_hbm.at[0], win), (wout_hbm.at[0], wout)))
    ]
    for ld in loads:
        ld.start()

    barrier = pltpu.get_barrier_semaphore()

    inward = Exchange(me, 1, hop_i, (mid_i0, mid_i1, mid_i2), fin_i, send_i, recv_i, cols)
    back = Exchange(me, -1, hop_r, (mid_r0, mid_r1, mid_r2), fin_r, send_r, recv_r, cols)

    peers = [inward.peers[dim, d, core] for core in range(2) for dim in range(3) for d in (1, 2, 3)] + [inward.peers[0, 0, 1]]
    for to in peers:
        pl.semaphore_signal(barrier, inc=1, device_id=(0, to), device_id_type=MESH)

    pos = coords(me)
    for core in range(2):
        q = lax.broadcasted_iota(jnp.int32, (rows, n_exp), 0)
        e = lax.broadcasted_iota(jnp.int32, (rows, n_exp), 1)
        ez = ((q >> 7) + pos[0]) & 3
        ey = ((q >> 5) + pos[1]) & 3
        ex = ((q >> 3) + pos[2]) & 3
        ec = (pos[3] + core) & 1
        want = ez * 32 + ey * 8 + ex * 2 + ec
        place[core] = jnp.where(e == want, 1.0, 0.0).astype(BF16)

    def put_blocks(dst, c, value):
        for z in range(4):
            for y in range(4):
                at = (z * 4 + y) * 32
                xs = value[at : at + 32, :].reshape(4, 8, d_model).astype(BF16)
                p0, p1, p2 = (xs[:, :, p * cols : (p + 1) * cols] for p in range(NPART))
                dst[c, 0, pl.ds(0, 3), y, z] = p0[1:]
                dst[c, 0, 3, y, z] = p0[0]
                dst[c, 1, (y + 3) % 4, z] = p1
                dst[c, 2, (z + 3) % 4, :, y] = p2

    def select(m):
        cur = l_ref[m * half : (m + 1) * half, :]
        rk = jnp.full(cur.shape, 15.0, F32)
        for r in range(RANKS):
            top = jnp.max(cur, axis=0, keepdims=True)
            hit = cur == top
            rk = jnp.where(hit, float(r), rk)
            cur = jnp.where(hit, -1e30, cur)
            for g in range(8):
                at = g * 16 + m * RANKS + r
                tops[at : at + 1, :] = top
        rank[m] = rk.astype(BF16)

    def gather(c):
        m, core = c // 2, c % 2
        wide = dot_t(place[core], rank[m])
        r_of = (lax.broadcasted_iota(jnp.int32, wide.shape, 0) & 7).astype(F32)
        pick = jnp.where(wide == r_of, 1.0, 0.0).astype(BF16)
        put_blocks(hop_i, c, dot(pick, x_ref[m * half : (m + 1) * half, :]))

    def tell_copy(src, dst, phase, dim, d, core):
        pltpu.make_async_remote_copy(
            src, dst, tell_send.at[phase], tell_recv.at[phase], device_id=(0, inward.peers[dim, d, core]), device_id_type=MESH
        ).start()

    def tell_wait(sem, phase, ref):
        pltpu.make_async_copy(ref, ref, sem.at[phase]).wait()

    def tell_first():
        q = lax.broadcasted_iota(jnp.int32, (NDEV, n_exp), 0)
        e = lax.broadcasted_iota(jnp.int32, (NDEV, n_exp), 1)
        ex = ((q >> 5) + 1 + pos[2]) & 3
        ey = ((q >> 3) + pos[1]) & 3
        ez = ((q >> 1) + pos[0]) & 3
        ec = (q + pos[3]) & 1
        at = jnp.where(e == ez * 32 + ey * 8 + ex * 2 + ec, 1.0, 0.0).astype(BF16)
        hi, mid, low = (dot_t(at, v) for v in split3(tops[...]))
        tell_hop[0:4] = ((hi + mid) + low).reshape(4, 4, 4, 2, 1, n_exp)
        for d in (1, 3, 2):
            tell_copy(tell_hop.at[d - 1], tell_hop.at[3 + d], 0, 2, d, 0)

    def tell_second():
        tell_wait(tell_recv, 0, tell_hop.at[pl.ds(4, 3)])
        for d in (1, 3, 2):
            tell_copy(tell_hop.at[pl.ds(3, 4), d], tell_mid.at[d - 1], 1, 1, d, 0)

    def tell_third():
        tell_wait(tell_recv, 1, tell_mid)
        for core in range(2):
            for d in (1, 3, 2, 0):
                if core or d:
                    tell_copy(tell_hop.at[pl.ds(3, 4), 0, d, core], told.at[core, d, 0], 3 - core, 0, d, core)
                    tell_copy(tell_mid.at[:, :, d, core], told.at[core, d, pl.ds(1, 3)], 3 - core, 0, d, core)

    def owner_cut():
        for ref, sem in ((told.at[1], tell_recv.at[2]), (told.at[0, pl.ds(1, 3)], tell_recv.at[3])):
            pltpu.make_async_copy(ref, ref, sem).wait()
        told[0, 0, 0] = tell_hop[3:7, 0, 0, 0]
        told[0, 0, 1:4] = tell_mid[:, :, 0, 0]
        seen = told[...].reshape(NDEV, n_exp)
        lane = lax.broadcasted_iota(jnp.int32, (n_exp, n_exp), 1)
        row = lax.broadcasted_iota(jnp.int32, (n_exp, n_exp), 0)
        same = jnp.where((lane >> 3) == (row >> 3), 1.0, 0.0).astype(BF16)
        first = jnp.where(((row & 7) == 0) & (((lane >> 3) & 1) == ((row >> 3) & 1)), 1.0, 0.0).astype(BF16)
        group = (lax.broadcasted_iota(jnp.int32, (8, n_exp), 1) >> 4).astype(F32)
        base = jnp.full((8, n_exp), -8.0, F32)
        width = 2.0
        for _ in range(8):
            cand = base + group * width
            over = jnp.where(seen >= cand[0:1], 1.0, 0.0)
            cnt = jnp.sum(over, axis=0, keepdims=True)
            cnt = dot(jnp.broadcast_to(cnt, (8, n_exp)).astype(BF16), same)
            flag = jnp.where(cnt >= float(KEEP), 1.0, 0.0).astype(BF16)
            base = base + (dot(flag, first) - 1.0) * width
            width = width / 8.0
        chosen = jnp.where(seen >= base[0:1], 1.0, 0.0).astype(BF16)
        for core in range(2):
            q = lax.broadcasted_iota(jnp.int32, (rows, NDEV), 0)
            src = lax.broadcasted_iota(jnp.int32, (rows, NDEV), 1)
            wide = dot(jnp.where(src == (q >> 3) + core * 64, 1.0, 0.0).astype(BF16), chosen)
            for m in range(2):
                keep = jnp.where(src == (q & 7) + m * 8, wide, 0.0)
                mask[m * 2 + core] = jnp.sum(keep, axis=1, keepdims=True)

    def gates():
        for m in range(2):
            lg = l_ref[m * half : (m + 1) * half, :]
            ex = jnp.exp(lg - jnp.max(lg, axis=1, keepdims=True))
            terms = split3(ex / jnp.sum(ex, axis=1, keepdims=True))
            for core in range(2):
                wide = dot_t(rank[m], place[core])
                r_of = (lax.broadcasted_iota(jnp.int32, wide.shape, 1) & 7).astype(F32)
                hit = wide == r_of
                for i, term in enumerate(terms):
                    comb[m * 2 + core, i] = jnp.where(hit, dot_t(term, place[core]), 0.0).astype(BF16)

    def combine(c):
        m, core = c // 2, c % 2
        for p in range(NPART):
            back.arrived_part(c, p)
            at = slice(p * cols, (p + 1) * cols)
            y = fin_r[c, :, :, :, :, at].reshape(rows, cols)
            total = dot(comb[c, 0], y) + dot(comb[c, 1], y) + dot(comb[c, 2], y)
            if core == 0:
                yacc[m, :, at] = total
            else:
                both = x_ref[m * half : (m + 1) * half, at].astype(F32) + (yacc[m, :, at] + total)
                out_ref[m * half : (m + 1) * half, at] = both.astype(BF16)

    def more():
        gather(2)
        gather(3)

    loads[0].wait()
    tops[...] = jnp.zeros_like(tops)
    select(0)
    loads[1].wait()
    gather(0)
    pl.semaphore_wait(barrier, len(peers))
    inward.first(0)
    select(1)
    tell_first()
    gather(1)
    inward.first(1)
    inward.second(0)
    inward.second(1)
    more()
    tell_second()
    inward.third(0)
    inward.first(2)
    tell_third()
    inward.first(3)
    inward.third(1)
    loads[2].wait()
    loads[3].wait()

    during = {
        2: [lambda: inward.second(2), lambda: owner_cut()],
        4: [lambda: inward.second(3)],
        7: [lambda: inward.third(2)],
        11: [lambda: inward.third(3)],
        12: [lambda: back.second(0)],
        15: [lambda: back.second(1)],
        18: [lambda: back.third(0)],
        20: [lambda: back.third(1)],
    }

    def step(i, _):
        c, f = lax.div(i, FSTEPS), lax.rem(i, FSTEPS)
        for k in range(NCHUNK):
            @pl.when(i == k * FSTEPS)
            def _():
                inward.arrived(k)
                acc[...] = jnp.zeros_like(acc)

        at = pl.multiple_of(f * ftile, ftile)
        h = gelu(dot(fin_i[c].reshape(rows, d_model), win[:, pl.ds(at, ftile)])).astype(BF16)
        acc[...] += dot(h, wout[pl.ds(at, ftile), :])

        for k in range(NCHUNK):
            @pl.when(i == k * FSTEPS + FSTEPS - 1)
            def _():
                put_blocks(hop_r, k, jnp.where(mask[k] > 0.5, acc[...], 0.0))
                back.first(k)
        for at_i, todo in during.items():
            @pl.when(i == at_i)
            def _():
                for fn in todo:
                    fn()
        return 0

    lax.fori_loop(0, NCHUNK * FSTEPS, step, 0)

    back.second(2)
    back.second(3)
    gates()
    back.third(2)
    back.third(3)
    combine(0)
    combine(1)
    combine(2)
    combine(3)

    inward.drain()
    back.drain()
    tell_wait(tell_send, 0, tell_hop.at[pl.ds(4, 3)])
    tell_wait(tell_send, 1, tell_mid)
    for ref, sem in ((told.at[1], tell_send.at[2]), (told.at[0, pl.ds(1, 3)], tell_send.at[3])):
        pltpu.make_async_copy(ref, ref, sem).wait()


def layer(hidden, logits, w_in, w_out):
    tok, d_model = hidden.shape
    n_exp = logits.shape[1]
    ff = w_in.shape[2]
    cols = d_model // NPART
    half = tok // 2

    def path():
        mids = [
            pltpu.VMEM((NCHUNK, *((3, 4) if o[1] < o[0] else (4, 3)), 4, RANKS, cols), BF16) for o in ORDERS
        ]
        return [pltpu.VMEM((NCHUNK, NPART, 7, 4, 4, RANKS, cols), BF16), *mids, pltpu.VMEM((NCHUNK, 4, 4, 4, RANKS, d_model), BF16)]

    n_sem = NCHUNK * NPART * 3
    dma = pltpu.SemaphoreType.DMA
    return pl.pallas_call(
        kernel,
        out_shape=jax.ShapeDtypeStruct(hidden.shape, hidden.dtype),
        in_specs=[pl.BlockSpec(memory_space=pl.ANY)] * 4,
        out_specs=pl.BlockSpec(memory_space=pltpu.VMEM),
        scratch_shapes=[
            pltpu.VMEM((tok, d_model), BF16),
            pltpu.VMEM((tok, n_exp), F32),
            pltpu.VMEM((d_model, ff), BF16),
            pltpu.VMEM((ff, d_model), BF16),
            *path(),
            *path(),
            pltpu.VMEM((2, 512, n_exp), BF16),
            pltpu.VMEM((NCHUNK, 3, half, 512), BF16),
            pltpu.VMEM((NCHUNK, 512, 1), F32),
            pltpu.VMEM((n_exp, n_exp), F32),
            pltpu.VMEM((7, 4, 4, 2, 1, n_exp), F32),
            pltpu.VMEM((3, 4, 4, 2, 1, n_exp), F32),
            pltpu.VMEM((2, 4, 4, 4, 1, n_exp), F32),
            pltpu.VMEM((2, half, n_exp), BF16),
            pltpu.VMEM((512, d_model), F32),
            pltpu.VMEM((2, half, d_model), F32),
            dma((4,)),
            dma((n_sem,)),
            dma((n_sem,)),
            dma((n_sem,)),
            dma((n_sem,)),
            dma((4,)),
            dma((4,)),
        ],
        compiler_params=pltpu.CompilerParams(collective_id=0, has_side_effects=True, vmem_limit_bytes=52 << 20),
    )(pltpu.with_memory_space_constraint(hidden, pltpu.HBM), pltpu.with_memory_space_constraint(logits, pltpu.HBM), w_in, w_out)


def solution(mesh):
    tok = P(("dp", "ep"), None)
    exp = P("ep", None, None)
    return jax.shard_map(layer, mesh=mesh, in_specs=(tok, tok, exp, exp), out_specs=tok, check_vma=False)
```

```python
import functools
import math

import jax
import jax.numpy as jnp
from jax import lax
from jax.experimental import pallas as pl
from jax.experimental.pallas import tpu as pltpu
from jax.sharding import PartitionSpec as P

MESH = pl.DeviceIdType.MESH
BF16, F32 = jnp.bfloat16, jnp.float32
NDEV = 128
RANKS = 8
KEEP = 512
ORDERS = ((2, 1, 0), (1, 0, 2), (0, 2, 1))
NPART = 3
NCHUNK = 4
FSTEPS = 3


def coords(d):
    return lax.div(d, 32), lax.rem(lax.div(d, 8), 4), lax.rem(lax.div(d, 2), 4), lax.rem(d, 2)


def shifted(me, offs, core):
    pos = coords(me)
    z, y, x = (lax.rem(p + (o + 4), 4) for p, o in zip(pos[:3], offs))
    return (z * 4 + y) * 8 + x * 2 + lax.rem(pos[3] + core, 2)


def along(dim, step):
    return tuple(step if d == dim else 0 for d in range(3))


def gelu(v):
    inner = v * (0.7978845608028654 + 0.035677408136300125 * (v * v))
    half = 0.5 * v
    return half + half * jnp.tanh(inner)


def split3(v):
    a = v.astype(BF16)
    r = v - a.astype(F32)
    b = r.astype(BF16)
    c = (r - b.astype(F32)).astype(BF16)
    return a, b, c


def dot(a, b):
    return jnp.dot(a, b, preferred_element_type=F32)


def dot_t(a, b):
    return lax.dot_general(a, b, (((1,), (1,)), ((), ())), preferred_element_type=F32)


class Exchange:
    def __init__(self, me, sign, hop, mids, final, send_sem, recv_sem, cols):
        self.me, self.sign, self.hop, self.mids, self.final = me, sign, hop, mids, final
        self.send_sem, self.recv_sem, self.cols = send_sem, recv_sem, cols
        self.peers = {}
        for core in range(2):
            for dim in range(3):
                for d in range(4):
                    self.peers[dim, d, core] = shifted(me, along(dim, sign * d), core)

    def sem(self, c, p, phase):
        return (c * NPART + p) * 3 + phase

    def copy(self, src, dst, c, p, phase, d, core):
        to = self.peers[ORDERS[p][phase], d, core]
        k = self.sem(c, p, phase)
        pltpu.make_async_remote_copy(
            src, dst, self.send_sem.at[k], self.recv_sem.at[k], device_id=(0, to), device_id_type=MESH
        ).start()

    def mid_at(self, p, c, d1):
        mid = self.mids[p]
        if ORDERS[p][1] < ORDERS[p][0]:
            return mid.at[c, d1 - 1]
        return mid.at[c, :, d1 - 1]

    def final_at(self, c, p, pick):
        idx = tuple(pick[ORDERS[p].index(d)] for d in range(3))
        return self.final.at[(c, *idx, slice(None), pl.ds(p * self.cols, self.cols))]

    def send0(self, c, p):
        for d in (1, 3, 2):
            self.copy(self.hop.at[c, p, d - 1], self.hop.at[c, p, 3 + d], c, p, 0, d, 0)

    def send1(self, c, p):
        for d in (1, 3, 2):
            self.copy(self.hop.at[c, p, pl.ds(3, 4), d], self.mid_at(p, c, d), c, p, 1, d, 0)

    def send2(self, c, p):
        core = c % 2
        for d in (1, 3, 2, 0):
            if d == 0 and core == 0:
                continue
            self.copy(self.hop.at[c, p, pl.ds(3, 4), 0, d], self.final_at(c, p, (pl.ds(0, 4), 0, d)), c, p, 2, d, core)
            self.copy(self.mids[p].at[c, :, :, d], self.final_at(c, p, (pl.ds(0, 4), pl.ds(1, 3), d)), c, p, 2, d, core)

    def own(self, c, p):
        self.final_set(c, p, (pl.ds(0, 4), 0, 0), self.hop[c, p, pl.ds(3, 4), 0, 0])
        self.final_set(c, p, (pl.ds(0, 4), pl.ds(1, 3), 0), self.mids[p][c, :, :, 0])

    def final_set(self, c, p, pick, value):
        idx = tuple(pick[ORDERS[p].index(d)] for d in range(3))
        self.final[(c, *idx, slice(None), pl.ds(p * self.cols, self.cols))] = value

    def region(self, c, p, phase):
        if phase == 0:
            return self.hop.at[c, p, pl.ds(4, 3)]
        if phase == 1:
            return self.mids[p].at[c]
        part = pl.ds(0, 4) if c % 2 else pl.ds(1, 3)
        return self.final_at(c, p, (pl.ds(0, 4), pl.ds(0, 4), part))

    def wait_recv(self, c, p, phase):
        r = self.region(c, p, phase)
        pltpu.make_async_copy(r, r, self.recv_sem.at[self.sem(c, p, phase)]).wait()

    def wait_send(self, c, p, phase):
        r = self.region(c, p, phase)
        pltpu.make_async_copy(r, r, self.send_sem.at[self.sem(c, p, phase)]).wait()

    def first(self, c):
        for p in range(NPART):
            self.send0(c, p)

    def second(self, c):
        for p in range(NPART):
            self.wait_recv(c, p, 0)
            self.send1(c, p)

    def third(self, c):
        for p in range(NPART):
            self.wait_recv(c, p, 1)
            self.send2(c, p)

    def arrived_part(self, c, p):
        self.wait_recv(c, p, 2)
        if c % 2 == 0:
            self.own(c, p)

    def arrived(self, c):
        for p in range(NPART):
            self.arrived_part(c, p)

    def drain(self, chunks, phases=(0, 1, 2)):
        for c in chunks:
            for p in range(NPART):
                for phase in phases:
                    self.wait_send(c, p, phase)


def kernel(
    x_hbm, l_hbm, win_hbm, wout_hbm, out_ref,
    x_ref, l_ref, win, wout, hop_i, mid_i0, mid_i1, mid_i2, fin_i, hop_r, mid_r0, mid_r1, mid_r2, fin_r,
    place, comb, mask, tops, tell_hop, tell_mid, told, rank, acc, yacc,
    load_sem, send_i, recv_i, send_r, recv_r, tell_send, tell_recv,
):
    me = lax.axis_index("ep")
    half, n_exp = l_ref.shape[0] // 2, l_ref.shape[1]
    d_model, ff = win.shape
    cols = d_model // NPART
    ftile = ff // FSTEPS
    rows = 64 * RANKS

    loads = [
        pltpu.make_async_copy(s, d, load_sem.at[i])
        for i, (s, d) in enumerate(((l_hbm, l_ref), (x_hbm, x_ref), (win_hbm.at[0], win), (wout_hbm.at[0], wout)))
    ]
    for ld in loads:
        ld.start()

    barrier = pltpu.get_barrier_semaphore()

    inward = Exchange(me, 1, hop_i, (mid_i0, mid_i1, mid_i2), fin_i, send_i, recv_i, cols)
    back = Exchange(me, -1, hop_r, (mid_r0, mid_r1, mid_r2), fin_r, send_r, recv_r, cols)

    peers = [inward.peers[dim, d, core] for core in range(2) for dim in range(3) for d in (1, 2, 3)] + [inward.peers[0, 0, 1]]
    for to in peers:
        pl.semaphore_signal(barrier, inc=1, device_id=(0, to), device_id_type=MESH)

    pos = coords(me)
    for core in range(2):
        q = lax.broadcasted_iota(jnp.int32, (rows, n_exp), 0)
        e = lax.broadcasted_iota(jnp.int32, (rows, n_exp), 1)
        ez = ((q >> 7) + pos[0]) & 3
        ey = ((q >> 5) + pos[1]) & 3
        ex = ((q >> 3) + pos[2]) & 3
        ec = (pos[3] + core) & 1
        want = ez * 32 + ey * 8 + ex * 2 + ec
        place[core] = jnp.where(e == want, 1.0, 0.0).astype(BF16)

    def put_blocks(dst, c, value):
        for z in range(4):
            for y in range(4):
                at = (z * 4 + y) * 32
                xs = value[at : at + 32, :].reshape(4, 8, d_model).astype(BF16)
                p0, p1, p2 = (xs[:, :, p * cols : (p + 1) * cols] for p in range(NPART))
                dst[c, 0, pl.ds(0, 3), y, z] = p0[1:]
                dst[c, 0, 3, y, z] = p0[0]
                dst[c, 1, (y + 3) % 4, z] = p1
                dst[c, 2, (z + 3) % 4, :, y] = p2

    def select(m):
        cur = l_ref[m * half : (m + 1) * half, :]
        rk = jnp.full(cur.shape, 15.0, F32)
        for r in range(RANKS):
            top = jnp.max(cur, axis=0, keepdims=True)
            hit = cur == top
            rk = jnp.where(hit, float(r), rk)
            cur = jnp.where(hit, -1e30, cur)
            for g in range(8):
                at = g * 16 + m * RANKS + r
                tops[at : at + 1, :] = top
        rank[m] = rk.astype(BF16)

    def gather(c):
        m, core = c // 2, c % 2
        wide = dot_t(place[core], rank[m])
        r_of = (lax.broadcasted_iota(jnp.int32, wide.shape, 0) & 7).astype(F32)
        pick = jnp.where(wide == r_of, 1.0, 0.0).astype(BF16)
        put_blocks(hop_i, c, dot(pick, x_ref[m * half : (m + 1) * half, :]))

    def tell_copy(src, dst, phase, dim, d, core):
        pltpu.make_async_remote_copy(
            src, dst, tell_send.at[phase], tell_recv.at[phase], device_id=(0, inward.peers[dim, d, core]), device_id_type=MESH
        ).start()

    def tell_wait(sem, phase, ref):
        pltpu.make_async_copy(ref, ref, sem.at[phase]).wait()

    def tell_first():
        q = lax.broadcasted_iota(jnp.int32, (NDEV, n_exp), 0)
        e = lax.broadcasted_iota(jnp.int32, (NDEV, n_exp), 1)
        ex = ((q >> 5) + 1 + pos[2]) & 3
        ey = ((q >> 3) + pos[1]) & 3
        ez = ((q >> 1) + pos[0]) & 3
        ec = (q + pos[3]) & 1
        at = jnp.where(e == ez * 32 + ey * 8 + ex * 2 + ec, 1.0, 0.0).astype(BF16)
        hi, mid, low = (dot_t(at, v) for v in split3(tops[...]))
        tell_hop[0:4] = ((hi + mid) + low).reshape(4, 4, 4, 2, 1, n_exp)
        for d in (1, 3, 2):
            tell_copy(tell_hop.at[d - 1], tell_hop.at[3 + d], 0, 2, d, 0)

    def tell_second():
        tell_wait(tell_recv, 0, tell_hop.at[pl.ds(4, 3)])
        for d in (1, 3, 2):
            tell_copy(tell_hop.at[pl.ds(3, 4), d], tell_mid.at[d - 1], 1, 1, d, 0)

    def tell_third():
        tell_wait(tell_recv, 1, tell_mid)
        for core in range(2):
            for d in (1, 3, 2, 0):
                if core or d:
                    tell_copy(tell_hop.at[pl.ds(3, 4), 0, d, core], told.at[core, d, 0], 3 - core, 0, d, core)
                    tell_copy(tell_mid.at[:, :, d, core], told.at[core, d, pl.ds(1, 3)], 3 - core, 0, d, core)

    def owner_cut():
        for ref, sem in ((told.at[1], tell_recv.at[2]), (told.at[0, pl.ds(1, 3)], tell_recv.at[3])):
            pltpu.make_async_copy(ref, ref, sem).wait()
        told[0, 0, 0] = tell_hop[3:7, 0, 0, 0]
        told[0, 0, 1:4] = tell_mid[:, :, 0, 0]
        seen = told[...].reshape(NDEV, n_exp)
        lane = lax.broadcasted_iota(jnp.int32, (n_exp, n_exp), 1)
        row = lax.broadcasted_iota(jnp.int32, (n_exp, n_exp), 0)
        same = jnp.where((lane >> 3) == (row >> 3), 1.0, 0.0).astype(BF16)
        first = jnp.where(((row & 7) == 0) & (((lane >> 3) & 1) == ((row >> 3) & 1)), 1.0, 0.0).astype(BF16)
        group = (lax.broadcasted_iota(jnp.int32, (8, n_exp), 1) >> 4).astype(F32)
        base = jnp.full((8, n_exp), -8.0, F32)
        width = 2.0
        for _ in range(8):
            cand = base + group * width
            over = jnp.where(seen >= cand[0:1], 1.0, 0.0)
            cnt = jnp.sum(over, axis=0, keepdims=True)
            cnt = dot(jnp.broadcast_to(cnt, (8, n_exp)).astype(BF16), same)
            flag = jnp.where(cnt >= float(KEEP), 1.0, 0.0).astype(BF16)
            base = base + (dot(flag, first) - 1.0) * width
            width = width / 8.0
        chosen = jnp.where(seen >= base[0:1], 1.0, 0.0).astype(BF16)
        for core in range(2):
            q = lax.broadcasted_iota(jnp.int32, (rows, NDEV), 0)
            src = lax.broadcasted_iota(jnp.int32, (rows, NDEV), 1)
            wide = dot(jnp.where(src == (q >> 3) + core * 64, 1.0, 0.0).astype(BF16), chosen)
            for m in range(2):
                keep = jnp.where(src == (q & 7) + m * 8, wide, 0.0)
                mask[m * 2 + core] = jnp.sum(keep, axis=1, keepdims=True)

    def gates():
        for m in range(2):
            lg = l_ref[m * half : (m + 1) * half, :]
            ex = jnp.exp(lg - jnp.max(lg, axis=1, keepdims=True))
            terms = split3(ex / jnp.sum(ex, axis=1, keepdims=True))
            for core in range(2):
                wide = dot_t(rank[m], place[core])
                r_of = (lax.broadcasted_iota(jnp.int32, wide.shape, 1) & 7).astype(F32)
                hit = wide == r_of
                for i, term in enumerate(terms):
                    comb[m * 2 + core, i] = jnp.where(hit, dot_t(term, place[core]), 0.0).astype(BF16)

    def drain_early():
        inward.drain(range(NCHUNK))
        tell_wait(tell_send, 0, tell_hop.at[pl.ds(4, 3)])
        tell_wait(tell_send, 1, tell_mid)
        for ref, sem in ((told.at[1], tell_send.at[2]), (told.at[0, pl.ds(1, 3)], tell_send.at[3])):
            pltpu.make_async_copy(ref, ref, sem).wait()

    def combine(c):
        m, core = c // 2, c % 2
        if c == 2:
            drain_early()
        if c == 3:
            back.drain(range(3))
            back.drain((3,), (0, 1))
        for p in range(NPART):
            back.arrived_part(c, p)
            at = slice(p * cols, (p + 1) * cols)
            y = fin_r[c, :, :, :, :, at].reshape(rows, cols)
            total = dot(comb[c, 0], y) + dot(comb[c, 1], y) + dot(comb[c, 2], y)
            if core == 0:
                yacc[m, :, at] = total
            else:
                both = x_ref[m * half : (m + 1) * half, at].astype(F32) + (yacc[m, :, at] + total)
                out_ref[m * half : (m + 1) * half, at] = both.astype(BF16)

    def more():
        gather(2)
        gather(3)

    loads[0].wait()
    tops[...] = jnp.zeros_like(tops)
    select(0)
    loads[1].wait()
    gather(0)
    pl.semaphore_wait(barrier, len(peers))
    inward.first(0)
    select(1)
    tell_first()
    gather(1)
    inward.first(1)
    more()
    inward.first(3)
    tell_second()
    inward.second(0)
    inward.first(2)
    inward.second(1)
    tell_third()
    inward.third(0)
    inward.second(2)
    inward.third(1)
    inward.second(3)
    owner_cut()
    loads[2].wait()
    loads[3].wait()

    during = {
        1: [lambda: inward.third(2)],
        4: [lambda: inward.third(3)],
        7: [lambda: back.second(0)],
        9: [lambda: back.second(1)],
    }

    def step(i, _):
        c, f = lax.div(i, FSTEPS), lax.rem(i, FSTEPS)
        for k in range(NCHUNK):
            @pl.when(i == k * FSTEPS)
            def _():
                inward.arrived(k)
                acc[...] = jnp.zeros_like(acc)

        at = pl.multiple_of(f * ftile, ftile)
        h = gelu(dot(fin_i[c].reshape(rows, d_model), win[:, pl.ds(at, ftile)])).astype(BF16)
        acc[...] += dot(h, wout[pl.ds(at, ftile), :])

        for k in range(NCHUNK):
            @pl.when(i == k * FSTEPS + FSTEPS - 1)
            def _():
                put_blocks(hop_r, k, jnp.where(mask[k] > 0.5, acc[...], 0.0))
                back.first(k)
        for at_i, todo in during.items():
            @pl.when(i == at_i)
            def _():
                for fn in todo:
                    fn()
        return 0

    lax.fori_loop(0, NCHUNK * FSTEPS, step, 0)

    back.third(0)
    back.second(2)
    gates()
    back.second(3)
    back.third(1)
    combine(0)
    back.third(2)
    back.third(3)
    combine(1)
    combine(2)
    combine(3)

    back.drain((3,), (2,))


def layer(hidden, logits, w_in, w_out):
    tok, d_model = hidden.shape
    n_exp = logits.shape[1]
    ff = w_in.shape[2]
    cols = d_model // NPART
    half = tok // 2

    def path():
        mids = [
            pltpu.VMEM((NCHUNK, *((3, 4) if o[1] < o[0] else (4, 3)), 4, RANKS, cols), BF16) for o in ORDERS
        ]
        return [pltpu.VMEM((NCHUNK, NPART, 7, 4, 4, RANKS, cols), BF16), *mids, pltpu.VMEM((NCHUNK, 4, 4, 4, RANKS, d_model), BF16)]

    n_sem = NCHUNK * NPART * 3
    dma = pltpu.SemaphoreType.DMA
    return pl.pallas_call(
        kernel,
        out_shape=jax.ShapeDtypeStruct(hidden.shape, hidden.dtype),
        in_specs=[pl.BlockSpec(memory_space=pl.ANY)] * 4,
        out_specs=pl.BlockSpec(memory_space=pltpu.VMEM),
        scratch_shapes=[
            pltpu.VMEM((tok, d_model), BF16),
            pltpu.VMEM((tok, n_exp), F32),
            pltpu.VMEM((d_model, ff), BF16),
            pltpu.VMEM((ff, d_model), BF16),
            *path(),
            *path(),
            pltpu.VMEM((2, 512, n_exp), BF16),
            pltpu.VMEM((NCHUNK, 3, half, 512), BF16),
            pltpu.VMEM((NCHUNK, 512, 1), F32),
            pltpu.VMEM((n_exp, n_exp), F32),
            pltpu.VMEM((7, 4, 4, 2, 1, n_exp), F32),
            pltpu.VMEM((3, 4, 4, 2, 1, n_exp), F32),
            pltpu.VMEM((2, 4, 4, 4, 1, n_exp), F32),
            pltpu.VMEM((2, half, n_exp), BF16),
            pltpu.VMEM((512, d_model), F32),
            pltpu.VMEM((2, half, d_model), F32),
            dma((4,)),
            dma((n_sem,)),
            dma((n_sem,)),
            dma((n_sem,)),
            dma((n_sem,)),
            dma((4,)),
            dma((4,)),
        ],
        compiler_params=pltpu.CompilerParams(collective_id=0, has_side_effects=True, vmem_limit_bytes=52 << 20),
    )(pltpu.with_memory_space_constraint(hidden, pltpu.HBM), pltpu.with_memory_space_constraint(logits, pltpu.HBM), w_in, w_out)


def solution(mesh):
    tok = P(("dp", "ep"), None)
    exp = P("ep", None, None)
    return jax.shard_map(layer, mesh=mesh, in_specs=(tok, tok, exp, exp), out_specs=tok, check_vma=False)
```

```python
import functools
import math

import jax
import jax.numpy as jnp
from jax import lax
from jax.experimental import pallas as pl
from jax.experimental.pallas import tpu as pltpu
from jax.sharding import PartitionSpec as P

MESH = pl.DeviceIdType.MESH
BF16, F32 = jnp.bfloat16, jnp.float32
NDEV = 128
RANKS = 8
KEEP = 512
ORDERS = ((2, 1, 0), (1, 0, 2), (0, 2, 1))
NPART = 3
NCHUNK = 4
FSTEPS = 3


def coords(d):
    return lax.div(d, 32), lax.rem(lax.div(d, 8), 4), lax.rem(lax.div(d, 2), 4), lax.rem(d, 2)


def shifted(me, offs, core):
    pos = coords(me)
    z, y, x = (lax.rem(p + (o + 4), 4) for p, o in zip(pos[:3], offs))
    return (z * 4 + y) * 8 + x * 2 + lax.rem(pos[3] + core, 2)


def along(dim, step):
    return tuple(step if d == dim else 0 for d in range(3))


def gelu(v):
    inner = v * (0.7978845608028654 + 0.035677408136300125 * (v * v))
    half = 0.5 * v
    return half + half * jnp.tanh(inner)


def split3(v):
    a = v.astype(BF16)
    r = v - a.astype(F32)
    b = r.astype(BF16)
    c = (r - b.astype(F32)).astype(BF16)
    return a, b, c


def dot(a, b):
    return jnp.dot(a, b, preferred_element_type=F32)


def dot_t(a, b):
    return lax.dot_general(a, b, (((1,), (1,)), ((), ())), preferred_element_type=F32)


class Exchange:
    def __init__(self, me, sign, hop, mids, final, send_sem, recv_sem, cols):
        self.me, self.sign, self.hop, self.mids, self.final = me, sign, hop, mids, final
        self.send_sem, self.recv_sem, self.cols = send_sem, recv_sem, cols
        self.peers = {}
        for core in range(2):
            for dim in range(3):
                for d in range(4):
                    self.peers[dim, d, core] = shifted(me, along(dim, sign * d), core)

    def sem(self, c, p, phase):
        return (c * NPART + p) * 3 + phase

    def copy(self, src, dst, c, p, phase, d, core):
        to = self.peers[ORDERS[p][phase], d, core]
        k = self.sem(c, p, phase)
        pltpu.make_async_remote_copy(
            src, dst, self.send_sem.at[k], self.recv_sem.at[k], device_id=(0, to), device_id_type=MESH
        ).start()

    def mid_at(self, p, c, d1):
        mid = self.mids[p]
        if ORDERS[p][1] < ORDERS[p][0]:
            return mid.at[c, d1 - 1]
        return mid.at[c, :, d1 - 1]

    def final_at(self, c, p, pick):
        idx = tuple(pick[ORDERS[p].index(d)] for d in range(3))
        return self.final.at[(c, *idx, slice(None), pl.ds(p * self.cols, self.cols))]

    def send0(self, c, p):
        for d in (2, 1, 3):
            self.copy(self.hop.at[c, p, d - 1], self.hop.at[c, p, 3 + d], c, p, 0, d, 0)

    def send1(self, c, p):
        for d in (2, 1, 3):
            self.copy(self.hop.at[c, p, pl.ds(3, 4), d], self.mid_at(p, c, d), c, p, 1, d, 0)

    def send2(self, c, p):
        core = c % 2
        for d in (2, 1, 3, 0):
            if d == 0 and core == 0:
                continue
            self.copy(self.hop.at[c, p, pl.ds(3, 4), 0, d], self.final_at(c, p, (pl.ds(0, 4), 0, d)), c, p, 2, d, core)
            self.copy(self.mids[p].at[c, :, :, d], self.final_at(c, p, (pl.ds(0, 4), pl.ds(1, 3), d)), c, p, 2, d, core)

    def own(self, c, p):
        self.final_set(c, p, (pl.ds(0, 4), 0, 0), self.hop[c, p, pl.ds(3, 4), 0, 0])
        self.final_set(c, p, (pl.ds(0, 4), pl.ds(1, 3), 0), self.mids[p][c, :, :, 0])

    def final_set(self, c, p, pick, value):
        idx = tuple(pick[ORDERS[p].index(d)] for d in range(3))
        self.final[(c, *idx, slice(None), pl.ds(p * self.cols, self.cols))] = value

    def region(self, c, p, phase):
        if phase == 0:
            return self.hop.at[c, p, pl.ds(4, 3)]
        if phase == 1:
            return self.mids[p].at[c]
        part = pl.ds(0, 4) if c % 2 else pl.ds(1, 3)
        return self.final_at(c, p, (pl.ds(0, 4), pl.ds(0, 4), part))

    def wait_recv(self, c, p, phase):
        r = self.region(c, p, phase)
        pltpu.make_async_copy(r, r, self.recv_sem.at[self.sem(c, p, phase)]).wait()

    def wait_send(self, c, p, phase):
        r = self.region(c, p, phase)
        pltpu.make_async_copy(r, r, self.send_sem.at[self.sem(c, p, phase)]).wait()

    def first(self, c):
        for p in range(NPART):
            self.send0(c, p)

    def second(self, c):
        for p in range(NPART):
            self.wait_recv(c, p, 0)
            self.send1(c, p)

    def third(self, c):
        for p in range(NPART):
            self.wait_recv(c, p, 1)
            self.send2(c, p)

    def arrived_part(self, c, p):
        self.wait_recv(c, p, 2)
        if c % 2 == 0:
            self.own(c, p)

    def arrived(self, c):
        for p in range(NPART):
            self.arrived_part(c, p)

    def drain(self, chunks, phases=(0, 1, 2)):
        for c in chunks:
            for p in range(NPART):
                for phase in phases:
                    self.wait_send(c, p, phase)


def kernel(
    x_hbm, l_hbm, win_hbm, wout_hbm, out_ref,
    x_ref, l_ref, win, wout, hop_i, mid_i0, mid_i1, mid_i2, fin_i, hop_r, mid_r0, mid_r1, mid_r2, fin_r,
    place, comb, mask, tops, tell_hop, tell_mid, told, rank, acc, yacc,
    load_sem, send_i, recv_i, send_r, recv_r, tell_send, tell_recv,
):
    me = lax.axis_index("ep")
    half, n_exp = l_ref.shape[0] // 2, l_ref.shape[1]
    d_model, ff = win.shape
    cols = d_model // NPART
    ftile = ff // FSTEPS
    rows = 64 * RANKS

    loads = [
        pltpu.make_async_copy(s, d, load_sem.at[i])
        for i, (s, d) in enumerate(((l_hbm, l_ref), (x_hbm, x_ref), (win_hbm.at[0], win), (wout_hbm.at[0], wout)))
    ]
    for ld in loads:
        ld.start()

    barrier = pltpu.get_barrier_semaphore()

    inward = Exchange(me, 1, hop_i, (mid_i0, mid_i1, mid_i2), fin_i, send_i, recv_i, cols)
    back = Exchange(me, -1, hop_r, (mid_r0, mid_r1, mid_r2), fin_r, send_r, recv_r, cols)

    peers = [inward.peers[dim, d, core] for core in range(2) for dim in range(3) for d in (1, 2, 3)] + [inward.peers[0, 0, 1]]
    for to in peers:
        pl.semaphore_signal(barrier, inc=1, device_id=(0, to), device_id_type=MESH)

    pos = coords(me)
    for core in range(2):
        q = lax.broadcasted_iota(jnp.int32, (rows, n_exp), 0)
        e = lax.broadcasted_iota(jnp.int32, (rows, n_exp), 1)
        ez = ((q >> 7) + pos[0]) & 3
        ey = ((q >> 5) + pos[1]) & 3
        ex = ((q >> 3) + pos[2]) & 3
        ec = (pos[3] + core) & 1
        want = ez * 32 + ey * 8 + ex * 2 + ec
        place[core] = jnp.where(e == want, 1.0, 0.0).astype(BF16)

    def put_blocks(dst, c, value):
        for z in range(4):
            for y in range(4):
                at = (z * 4 + y) * 32
                xs = value[at : at + 32, :].reshape(4, 8, d_model).astype(BF16)
                p0, p1, p2 = (xs[:, :, p * cols : (p + 1) * cols] for p in range(NPART))
                dst[c, 0, pl.ds(0, 3), y, z] = p0[1:]
                dst[c, 0, 3, y, z] = p0[0]
                dst[c, 1, (y + 3) % 4, z] = p1
                dst[c, 2, (z + 3) % 4, :, y] = p2

    def select(m):
        cur = l_ref[m * half : (m + 1) * half, :]
        rk = jnp.full(cur.shape, 15.0, F32)
        for r in range(RANKS):
            top = jnp.max(cur, axis=0, keepdims=True)
            hit = cur == top
            rk = jnp.where(hit, float(r), rk)
            cur = jnp.where(hit, -1e30, cur)
            for g in range(8):
                at = g * 16 + m * RANKS + r
                tops[at : at + 1, :] = top
        rank[m] = rk.astype(BF16)

    def gather(c):
        m, core = c // 2, c % 2
        wide = dot_t(place[core], rank[m])
        r_of = (lax.broadcasted_iota(jnp.int32, wide.shape, 0) & 7).astype(F32)
        pick = jnp.where(wide == r_of, 1.0, 0.0).astype(BF16)
        put_blocks(hop_i, c, dot(pick, x_ref[m * half : (m + 1) * half, :]))

    def tell_copy(src, dst, phase, dim, d, core):
        pltpu.make_async_remote_copy(
            src, dst, tell_send.at[phase], tell_recv.at[phase], device_id=(0, inward.peers[dim, d, core]), device_id_type=MESH
        ).start()

    def tell_wait(sem, phase, ref):
        pltpu.make_async_copy(ref, ref, sem.at[phase]).wait()

    def tell_first():
        q = lax.broadcasted_iota(jnp.int32, (NDEV, n_exp), 0)
        e = lax.broadcasted_iota(jnp.int32, (NDEV, n_exp), 1)
        ex = ((q >> 5) + 1 + pos[2]) & 3
        ey = ((q >> 3) + pos[1]) & 3
        ez = ((q >> 1) + pos[0]) & 3
        ec = (q + pos[3]) & 1
        at = jnp.where(e == ez * 32 + ey * 8 + ex * 2 + ec, 1.0, 0.0).astype(BF16)
        hi, mid, low = (dot_t(at, v) for v in split3(tops[...]))
        tell_hop[0:4] = ((hi + mid) + low).reshape(4, 4, 4, 2, 1, n_exp)
        for d in (2, 1, 3):
            tell_copy(tell_hop.at[d - 1], tell_hop.at[3 + d], 0, 2, d, 0)

    def tell_second():
        tell_wait(tell_recv, 0, tell_hop.at[pl.ds(4, 3)])
        for d in (2, 1, 3):
            tell_copy(tell_hop.at[pl.ds(3, 4), d], tell_mid.at[d - 1], 1, 1, d, 0)

    def tell_third():
        tell_wait(tell_recv, 1, tell_mid)
        for core in range(2):
            for d in (2, 1, 3, 0):
                if core or d:
                    tell_copy(tell_hop.at[pl.ds(3, 4), 0, d, core], told.at[core, d, 0], 3 - core, 0, d, core)
                    tell_copy(tell_mid.at[:, :, d, core], told.at[core, d, pl.ds(1, 3)], 3 - core, 0, d, core)

    def owner_cut():
        for ref, sem in ((told.at[1], tell_recv.at[2]), (told.at[0, pl.ds(1, 3)], tell_recv.at[3])):
            pltpu.make_async_copy(ref, ref, sem).wait()
        told[0, 0, 0] = tell_hop[3:7, 0, 0, 0]
        told[0, 0, 1:4] = tell_mid[:, :, 0, 0]
        seen = told[...].reshape(NDEV, n_exp)
        lane = lax.broadcasted_iota(jnp.int32, (n_exp, n_exp), 1)
        row = lax.broadcasted_iota(jnp.int32, (n_exp, n_exp), 0)
        same = jnp.where((lane >> 3) == (row >> 3), 1.0, 0.0).astype(BF16)
        first = jnp.where(((row & 7) == 0) & (((lane >> 3) & 1) == ((row >> 3) & 1)), 1.0, 0.0).astype(BF16)
        group = (lax.broadcasted_iota(jnp.int32, (8, n_exp), 1) >> 4).astype(F32)
        base = jnp.full((8, n_exp), -8.0, F32)
        width = 2.0
        for _ in range(8):
            cand = base + group * width
            over = jnp.where(seen >= cand[0:1], 1.0, 0.0)
            cnt = jnp.sum(over, axis=0, keepdims=True)
            cnt = dot(jnp.broadcast_to(cnt, (8, n_exp)).astype(BF16), same)
            flag = jnp.where(cnt >= float(KEEP), 1.0, 0.0).astype(BF16)
            base = base + (dot(flag, first) - 1.0) * width
            width = width / 8.0
        chosen = jnp.where(seen >= base[0:1], 1.0, 0.0).astype(BF16)
        for core in range(2):
            q = lax.broadcasted_iota(jnp.int32, (rows, NDEV), 0)
            src = lax.broadcasted_iota(jnp.int32, (rows, NDEV), 1)
            wide = dot(jnp.where(src == (q >> 3) + core * 64, 1.0, 0.0).astype(BF16), chosen)
            for m in range(2):
                keep = jnp.where(src == (q & 7) + m * 8, wide, 0.0)
                mask[m * 2 + core] = jnp.sum(keep, axis=1, keepdims=True)

    def gates():
        for m in range(2):
            lg = l_ref[m * half : (m + 1) * half, :]
            ex = jnp.exp(lg - jnp.max(lg, axis=1, keepdims=True))
            terms = split3(ex / jnp.sum(ex, axis=1, keepdims=True))
            for core in range(2):
                wide = dot_t(rank[m], place[core])
                r_of = (lax.broadcasted_iota(jnp.int32, wide.shape, 1) & 7).astype(F32)
                hit = wide == r_of
                for i, term in enumerate(terms):
                    comb[m * 2 + core, i] = jnp.where(hit, dot_t(term, place[core]), 0.0).astype(BF16)

    def drain_early():
        inward.drain(range(NCHUNK))
        tell_wait(tell_send, 0, tell_hop.at[pl.ds(4, 3)])
        tell_wait(tell_send, 1, tell_mid)
        for ref, sem in ((told.at[1], tell_send.at[2]), (told.at[0, pl.ds(1, 3)], tell_send.at[3])):
            pltpu.make_async_copy(ref, ref, sem).wait()

    def combine(c):
        m, core = c // 2, c % 2
        if c == 2:
            drain_early()
        if c == 3:
            back.drain(range(3))
            back.drain((3,), (0, 1))
        for p in range(NPART):
            back.arrived_part(c, p)
            at = slice(p * cols, (p + 1) * cols)
            y = fin_r[c, :, :, :, :, at].reshape(rows, cols)
            total = dot(comb[c, 0], y) + dot(comb[c, 1], y) + dot(comb[c, 2], y)
            if core == 0:
                yacc[m, :, at] = total
            else:
                both = x_ref[m * half : (m + 1) * half, at].astype(F32) + (yacc[m, :, at] + total)
                out_ref[m * half : (m + 1) * half, at] = both.astype(BF16)

    def more():
        gather(2)
        gather(3)

    loads[0].wait()
    tops[...] = jnp.zeros_like(tops)
    select(0)
    loads[1].wait()
    gather(0)
    pl.semaphore_wait(barrier, len(peers))
    inward.first(0)
    select(1)
    tell_first()
    gather(1)
    inward.first(1)
    more()
    inward.first(3)
    tell_second()
    inward.second(0)
    inward.first(2)
    inward.second(1)
    tell_third()
    inward.third(0)
    inward.second(2)
    inward.third(1)
    inward.second(3)
    owner_cut()
    loads[2].wait()
    loads[3].wait()

    during = {
        1: [lambda: inward.third(2)],
        4: [lambda: inward.third(3)],
        7: [lambda: back.second(0)],
        9: [lambda: back.second(1)],
    }

    def step(i, _):
        c, f = lax.div(i, FSTEPS), lax.rem(i, FSTEPS)
        for k in range(NCHUNK):
            @pl.when(i == k * FSTEPS)
            def _():
                inward.arrived(k)
                acc[...] = jnp.zeros_like(acc)

        at = pl.multiple_of(f * ftile, ftile)
        h = gelu(dot(fin_i[c].reshape(rows, d_model), win[:, pl.ds(at, ftile)])).astype(BF16)
        acc[...] += dot(h, wout[pl.ds(at, ftile), :])

        for k in range(NCHUNK):
            @pl.when(i == k * FSTEPS + FSTEPS - 1)
            def _():
                put_blocks(hop_r, k, jnp.where(mask[k] > 0.5, acc[...], 0.0))
                back.first(k)
        for at_i, todo in during.items():
            @pl.when(i == at_i)
            def _():
                for fn in todo:
                    fn()
        return 0

    lax.fori_loop(0, NCHUNK * FSTEPS, step, 0)

    back.third(0)
    back.second(2)
    gates()
    back.second(3)
    back.third(1)
    combine(0)
    back.third(2)
    back.third(3)
    combine(1)
    combine(2)
    combine(3)

    back.drain((3,), (2,))


def layer(hidden, logits, w_in, w_out):
    tok, d_model = hidden.shape
    n_exp = logits.shape[1]
    ff = w_in.shape[2]
    cols = d_model // NPART
    half = tok // 2

    def path():
        mids = [
            pltpu.VMEM((NCHUNK, *((3, 4) if o[1] < o[0] else (4, 3)), 4, RANKS, cols), BF16) for o in ORDERS
        ]
        return [pltpu.VMEM((NCHUNK, NPART, 7, 4, 4, RANKS, cols), BF16), *mids, pltpu.VMEM((NCHUNK, 4, 4, 4, RANKS, d_model), BF16)]

    n_sem = NCHUNK * NPART * 3
    dma = pltpu.SemaphoreType.DMA
    return pl.pallas_call(
        kernel,
        out_shape=jax.ShapeDtypeStruct(hidden.shape, hidden.dtype),
        in_specs=[pl.BlockSpec(memory_space=pl.ANY)] * 4,
        out_specs=pl.BlockSpec(memory_space=pltpu.VMEM),
        scratch_shapes=[
            pltpu.VMEM((tok, d_model), BF16),
            pltpu.VMEM((tok, n_exp), F32),
            pltpu.VMEM((d_model, ff), BF16),
            pltpu.VMEM((ff, d_model), BF16),
            *path(),
            *path(),
            pltpu.VMEM((2, 512, n_exp), BF16),
            pltpu.VMEM((NCHUNK, 3, half, 512), BF16),
            pltpu.VMEM((NCHUNK, 512, 1), F32),
            pltpu.VMEM((n_exp, n_exp), F32),
            pltpu.VMEM((7, 4, 4, 2, 1, n_exp), F32),
            pltpu.VMEM((3, 4, 4, 2, 1, n_exp), F32),
            pltpu.VMEM((2, 4, 4, 4, 1, n_exp), F32),
            pltpu.VMEM((2, half, n_exp), BF16),
            pltpu.VMEM((512, d_model), F32),
            pltpu.VMEM((2, half, d_model), F32),
            dma((4,)),
            dma((n_sem,)),
            dma((n_sem,)),
            dma((n_sem,)),
            dma((n_sem,)),
            dma((4,)),
            dma((4,)),
        ],
        compiler_params=pltpu.CompilerParams(collective_id=0, has_side_effects=True, vmem_limit_bytes=52 << 20),
    )(pltpu.with_memory_space_constraint(hidden, pltpu.HBM), pltpu.with_memory_space_constraint(logits, pltpu.HBM), w_in, w_out)


def solution(mesh):
    tok = P(("dp", "ep"), None)
    exp = P("ep", None, None)
    return jax.shard_map(layer, mesh=mesh, in_specs=(tok, tok, exp, exp), out_specs=tok, check_vma=False)
```

```python
import functools
import math

import jax
import jax.numpy as jnp
from jax import lax
from jax.experimental import pallas as pl
from jax.experimental.pallas import tpu as pltpu
from jax.sharding import PartitionSpec as P

MESH = pl.DeviceIdType.MESH
BF16, F32 = jnp.bfloat16, jnp.float32
NDEV = 128
RANKS = 8
KEEP = 512
ORDERS = ((2, 1, 0), (1, 0, 2), (0, 2, 1))
NPART = 3
NCHUNK = 4
FSTEPS = 3


def coords(d):
    return lax.div(d, 32), lax.rem(lax.div(d, 8), 4), lax.rem(lax.div(d, 2), 4), lax.rem(d, 2)


def shifted(me, offs, core):
    pos = coords(me)
    z, y, x = (lax.rem(p + (o + 4), 4) for p, o in zip(pos[:3], offs))
    return (z * 4 + y) * 8 + x * 2 + lax.rem(pos[3] + core, 2)


def along(dim, step):
    return tuple(step if d == dim else 0 for d in range(3))


def gelu(v):
    inner = v * (0.7978845608028654 + 0.035677408136300125 * (v * v))
    half = 0.5 * v
    return half + half * jnp.tanh(inner)


def split3(v):
    a = v.astype(BF16)
    r = v - a.astype(F32)
    b = r.astype(BF16)
    c = (r - b.astype(F32)).astype(BF16)
    return a, b, c


def dot(a, b):
    return jnp.dot(a, b, preferred_element_type=F32)


def dot_t(a, b):
    return lax.dot_general(a, b, (((1,), (1,)), ((), ())), preferred_element_type=F32)


class Exchange:
    def __init__(self, me, sign, hop, mids, final, send_sem, recv_sem, cols):
        self.me, self.sign, self.hop, self.mids, self.final = me, sign, hop, mids, final
        self.send_sem, self.recv_sem, self.cols = send_sem, recv_sem, cols
        self.peers = {}
        for core in range(2):
            for dim in range(3):
                for d in range(4):
                    self.peers[dim, d, core] = shifted(me, along(dim, sign * d), core)

    def sem(self, c, p, phase):
        return (c * NPART + p) * 3 + phase

    def copy(self, src, dst, c, p, phase, d, core):
        to = self.peers[ORDERS[p][phase], d, core]
        k = self.sem(c, p, phase)
        pltpu.make_async_remote_copy(
            src, dst, self.send_sem.at[k], self.recv_sem.at[k], device_id=(0, to), device_id_type=MESH
        ).start()

    def mid_at(self, p, c, d1):
        mid = self.mids[p]
        if ORDERS[p][1] < ORDERS[p][0]:
            return mid.at[c, d1 - 1]
        return mid.at[c, :, d1 - 1]

    def final_at(self, c, p, pick):
        idx = tuple(pick[ORDERS[p].index(d)] for d in range(3))
        return self.final.at[(c, *idx, slice(None), pl.ds(p * self.cols, self.cols))]

    def send0(self, c, p):
        for d in (2, 1, 3):
            self.copy(self.hop.at[c, p, d - 1], self.hop.at[c, p, 3 + d], c, p, 0, d, 0)

    def send1(self, c, p):
        for d in (2, 1, 3):
            self.copy(self.hop.at[c, p, pl.ds(3, 4), d], self.mid_at(p, c, d), c, p, 1, d, 0)

    def send2(self, c, p):
        core = c % 2
        for d in (2, 1, 3, 0):
            if d == 0 and core == 0:
                continue
            self.copy(self.hop.at[c, p, pl.ds(3, 4), 0, d], self.final_at(c, p, (pl.ds(0, 4), 0, d)), c, p, 2, d, core)
            self.copy(self.mids[p].at[c, :, :, d], self.final_at(c, p, (pl.ds(0, 4), pl.ds(1, 3), d)), c, p, 2, d, core)

    def own(self, c, p):
        self.final_set(c, p, (pl.ds(0, 4), 0, 0), self.hop[c, p, pl.ds(3, 4), 0, 0])
        self.final_set(c, p, (pl.ds(0, 4), pl.ds(1, 3), 0), self.mids[p][c, :, :, 0])

    def final_set(self, c, p, pick, value):
        idx = tuple(pick[ORDERS[p].index(d)] for d in range(3))
        self.final[(c, *idx, slice(None), pl.ds(p * self.cols, self.cols))] = value

    def region(self, c, p, phase):
        if phase == 0:
            return self.hop.at[c, p, pl.ds(4, 3)]
        if phase == 1:
            return self.mids[p].at[c]
        part = pl.ds(0, 4) if c % 2 else pl.ds(1, 3)
        return self.final_at(c, p, (pl.ds(0, 4), pl.ds(0, 4), part))

    def wait_recv(self, c, p, phase):
        r = self.region(c, p, phase)
        pltpu.make_async_copy(r, r, self.recv_sem.at[self.sem(c, p, phase)]).wait()

    def wait_send(self, c, p, phase):
        r = self.region(c, p, phase)
        pltpu.make_async_copy(r, r, self.send_sem.at[self.sem(c, p, phase)]).wait()

    def first(self, c):
        for p in range(NPART):
            self.send0(c, p)

    def second(self, c):
        for p in range(NPART):
            self.wait_recv(c, p, 0)
            self.send1(c, p)

    def third(self, c):
        for p in range(NPART):
            self.wait_recv(c, p, 1)
            self.send2(c, p)

    def arrived_part(self, c, p):
        self.wait_recv(c, p, 2)
        if c % 2 == 0:
            self.own(c, p)

    def arrived(self, c):
        for p in range(NPART):
            self.arrived_part(c, p)

    def drain(self, chunks, phases=(0, 1, 2)):
        for c in chunks:
            for p in range(NPART):
                for phase in phases:
                    self.wait_send(c, p, phase)


def kernel(
    x_hbm, l_hbm, win_hbm, wout_hbm, out_ref,
    x_ref, l_ref, win, wout, hop_i, mid_i0, mid_i1, mid_i2, fin_i, hop_r, mid_r0, mid_r1, mid_r2, fin_r,
    place, comb, mask, tops, tell_hop, tell_mid, told, rank, acc, yacc,
    load_sem, send_i, recv_i, send_r, recv_r, tell_send, tell_recv,
):
    me = lax.axis_index("ep")
    half, n_exp = l_ref.shape[0] // 2, l_ref.shape[1]
    d_model, ff = win.shape
    cols = d_model // NPART
    ftile = ff // FSTEPS
    rows = 64 * RANKS

    loads = [
        pltpu.make_async_copy(s, d, load_sem.at[i])
        for i, (s, d) in enumerate(((l_hbm, l_ref), (x_hbm, x_ref), (win_hbm.at[0], win), (wout_hbm.at[0], wout)))
    ]
    for ld in loads:
        ld.start()

    barrier = pltpu.get_barrier_semaphore()

    inward = Exchange(me, 1, hop_i, (mid_i0, mid_i1, mid_i2), fin_i, send_i, recv_i, cols)
    back = Exchange(me, -1, hop_r, (mid_r0, mid_r1, mid_r2), fin_r, send_r, recv_r, cols)

    peers = [inward.peers[dim, d, core] for core in range(2) for dim in range(3) for d in (1, 2, 3)] + [inward.peers[0, 0, 1]]
    for to in peers:
        pl.semaphore_signal(barrier, inc=1, device_id=(0, to), device_id_type=MESH)

    pos = coords(me)
    for core in range(2):
        q = lax.broadcasted_iota(jnp.int32, (rows, n_exp), 0)
        e = lax.broadcasted_iota(jnp.int32, (rows, n_exp), 1)
        ez = ((q >> 7) + pos[0]) & 3
        ey = ((q >> 5) + pos[1]) & 3
        ex = ((q >> 3) + pos[2]) & 3
        ec = (pos[3] + core) & 1
        want = ez * 32 + ey * 8 + ex * 2 + ec
        place[core] = jnp.where(e == want, 1.0, 0.0).astype(BF16)

    def put_blocks(dst, c, value):
        for z in range(4):
            for y in range(4):
                at = (z * 4 + y) * 32
                xs = value[at : at + 32, :].reshape(4, 8, d_model).astype(BF16)
                p0, p1, p2 = (xs[:, :, p * cols : (p + 1) * cols] for p in range(NPART))
                dst[c, 0, pl.ds(0, 3), y, z] = p0[1:]
                dst[c, 0, 3, y, z] = p0[0]
                dst[c, 1, (y + 3) % 4, z] = p1
                dst[c, 2, (z + 3) % 4, :, y] = p2

    def select(m):
        cur = l_ref[m * half : (m + 1) * half, :]
        rk = jnp.full(cur.shape, 15.0, F32)
        for r in range(RANKS):
            top = jnp.max(cur, axis=0, keepdims=True)
            hit = cur == top
            rk = jnp.where(hit, float(r), rk)
            cur = jnp.where(hit, -1e30, cur)
            for g in range(8):
                at = g * 16 + m * RANKS + r
                tops[at : at + 1, :] = top
        rank[m] = rk.astype(BF16)

    def gather(c):
        m, core = c // 2, c % 2
        wide = dot_t(place[core], rank[m])
        r_of = (lax.broadcasted_iota(jnp.int32, wide.shape, 0) & 7).astype(F32)
        pick = jnp.where(wide == r_of, 1.0, 0.0).astype(BF16)
        put_blocks(hop_i, c, dot(pick, x_ref[m * half : (m + 1) * half, :]))

    def tell_copy(src, dst, phase, dim, d, core):
        pltpu.make_async_remote_copy(
            src, dst, tell_send.at[phase], tell_recv.at[phase], device_id=(0, inward.peers[dim, d, core]), device_id_type=MESH
        ).start()

    def tell_wait(sem, phase, ref):
        pltpu.make_async_copy(ref, ref, sem.at[phase]).wait()

    def tell_first():
        q = lax.broadcasted_iota(jnp.int32, (NDEV, n_exp), 0)
        e = lax.broadcasted_iota(jnp.int32, (NDEV, n_exp), 1)
        ex = ((q >> 5) + 1 + pos[2]) & 3
        ey = ((q >> 3) + pos[1]) & 3
        ez = ((q >> 1) + pos[0]) & 3
        ec = (q + pos[3]) & 1
        at = jnp.where(e == ez * 32 + ey * 8 + ex * 2 + ec, 1.0, 0.0).astype(BF16)
        hi, mid, low = (dot_t(at, v) for v in split3(tops[...]))
        tell_hop[0:4] = ((hi + mid) + low).reshape(4, 4, 4, 2, 1, n_exp)
        for d in (2, 1, 3):
            tell_copy(tell_hop.at[d - 1], tell_hop.at[3 + d], 0, 2, d, 0)

    def tell_second():
        tell_wait(tell_recv, 0, tell_hop.at[pl.ds(4, 3)])
        for d in (2, 1, 3):
            tell_copy(tell_hop.at[pl.ds(3, 4), d], tell_mid.at[d - 1], 1, 1, d, 0)

    def tell_third():
        tell_wait(tell_recv, 1, tell_mid)
        for core in range(2):
            for d in (2, 1, 3, 0):
                if core or d:
                    tell_copy(tell_hop.at[pl.ds(3, 4), 0, d, core], told.at[core, d, 0], 3 - core, 0, d, core)
                    tell_copy(tell_mid.at[:, :, d, core], told.at[core, d, pl.ds(1, 3)], 3 - core, 0, d, core)

    def owner_cut():
        for ref, sem in ((told.at[1], tell_recv.at[2]), (told.at[0, pl.ds(1, 3)], tell_recv.at[3])):
            pltpu.make_async_copy(ref, ref, sem).wait()
        told[0, 0, 0] = tell_hop[3:7, 0, 0, 0]
        told[0, 0, 1:4] = tell_mid[:, :, 0, 0]
        seen = told[...].reshape(NDEV, n_exp)
        lane = lax.broadcasted_iota(jnp.int32, (n_exp, n_exp), 1)
        row = lax.broadcasted_iota(jnp.int32, (n_exp, n_exp), 0)
        same = jnp.where((lane >> 3) == (row >> 3), 1.0, 0.0).astype(BF16)
        first = jnp.where(((row & 7) == 0) & (((lane >> 3) & 1) == ((row >> 3) & 1)), 1.0, 0.0).astype(BF16)
        group = (lax.broadcasted_iota(jnp.int32, (8, n_exp), 1) >> 4).astype(F32)
        base = jnp.full((8, n_exp), -8.0, F32)
        width = 2.0
        for _ in range(8):
            cand = base + group * width
            over = jnp.where(seen >= cand[0:1], 1.0, 0.0)
            cnt = jnp.sum(over, axis=0, keepdims=True)
            cnt = dot(jnp.broadcast_to(cnt, (8, n_exp)).astype(BF16), same)
            flag = jnp.where(cnt >= float(KEEP), 1.0, 0.0).astype(BF16)
            base = base + (dot(flag, first) - 1.0) * width
            width = width / 8.0
        chosen = jnp.where(seen >= base[0:1], 1.0, 0.0).astype(BF16)
        for core in range(2):
            q = lax.broadcasted_iota(jnp.int32, (rows, NDEV), 0)
            src = lax.broadcasted_iota(jnp.int32, (rows, NDEV), 1)
            wide = dot(jnp.where(src == (q >> 3) + core * 64, 1.0, 0.0).astype(BF16), chosen)
            for m in range(2):
                keep = jnp.where(src == (q & 7) + m * 8, wide, 0.0)
                mask[m * 2 + core] = jnp.sum(keep, axis=1, keepdims=True)

    def gates():
        for m in range(2):
            lg = l_ref[m * half : (m + 1) * half, :]
            ex = jnp.exp(lg - jnp.max(lg, axis=1, keepdims=True))
            terms = split3(ex / jnp.sum(ex, axis=1, keepdims=True))
            for core in range(2):
                wide = dot_t(rank[m], place[core])
                r_of = (lax.broadcasted_iota(jnp.int32, wide.shape, 1) & 7).astype(F32)
                hit = wide == r_of
                for i, term in enumerate(terms):
                    comb[m * 2 + core, i] = jnp.where(hit, dot_t(term, place[core]), 0.0).astype(BF16)

    def drain_early():
        inward.drain(range(NCHUNK))
        tell_wait(tell_send, 0, tell_hop.at[pl.ds(4, 3)])
        tell_wait(tell_send, 1, tell_mid)
        for ref, sem in ((told.at[1], tell_send.at[2]), (told.at[0, pl.ds(1, 3)], tell_send.at[3])):
            pltpu.make_async_copy(ref, ref, sem).wait()

    def combine(c):
        m, core = c // 2, c % 2
        if c == 2:
            drain_early()
        if c == 3:
            back.drain(range(3))
            back.drain((3,), (0, 1))
        for p in range(NPART):
            back.arrived_part(c, p)
            at = slice(p * cols, (p + 1) * cols)
            y = fin_r[c, :, :, :, :, at].reshape(rows, cols)
            total = dot(comb[c, 0], y) + dot(comb[c, 1], y) + dot(comb[c, 2], y)
            if core == 0:
                yacc[m, :, at] = total
            else:
                both = x_ref[m * half : (m + 1) * half, at].astype(F32) + (yacc[m, :, at] + total)
                out_ref[m * half : (m + 1) * half, at] = both.astype(BF16)

    def more():
        gather(2)
        gather(3)

    loads[0].wait()
    tops[...] = jnp.zeros_like(tops)
    select(0)
    loads[1].wait()
    gather(0)
    pl.semaphore_wait(barrier, len(peers))
    inward.first(0)
    select(1)
    tell_first()
    gather(1)
    inward.first(1)
    more()
    gates()
    inward.first(3)
    tell_second()
    inward.second(0)
    inward.first(2)
    inward.second(1)
    tell_third()
    inward.third(0)
    inward.second(2)
    inward.third(1)
    inward.second(3)
    owner_cut()
    loads[2].wait()
    loads[3].wait()

    during = {
        1: [lambda: inward.third(2)],
        4: [lambda: inward.third(3)],
        6: [lambda: back.second(0)],
        9: [lambda: back.second(1)],
    }

    def step(i, _):
        c, f = lax.div(i, FSTEPS), lax.rem(i, FSTEPS)
        for k in range(NCHUNK):
            @pl.when(i == k * FSTEPS)
            def _():
                inward.arrived(k)
                acc[...] = jnp.zeros_like(acc)

        at = pl.multiple_of(f * ftile, ftile)
        chunk = fin_i[c].reshape(rows, d_model)
        cut = rows // 2
        up = [dot(chunk[r : r + cut], win[:, pl.ds(at, ftile)]) for r in (0, cut)]
        for r, pre in zip((0, cut), up):
            acc[r : r + cut] += dot(gelu(pre).astype(BF16), wout[pl.ds(at, ftile), :])

        for k in range(NCHUNK):
            @pl.when(i == k * FSTEPS + FSTEPS - 1)
            def _():
                put_blocks(hop_r, k, jnp.where(mask[k] > 0.5, acc[...], 0.0))
                back.first(k)
        for at_i, todo in during.items():
            @pl.when(i == at_i)
            def _():
                for fn in todo:
                    fn()
        return 0

    lax.fori_loop(0, NCHUNK * FSTEPS, step, 0)

    back.second(2)
    back.third(0)
    back.second(3)
    back.third(2)
    back.third(1)
    combine(0)
    back.third(3)
    combine(1)
    combine(2)
    combine(3)

    back.drain((3,), (2,))


def layer(hidden, logits, w_in, w_out):
    tok, d_model = hidden.shape
    n_exp = logits.shape[1]
    ff = w_in.shape[2]
    cols = d_model // NPART
    half = tok // 2

    def path():
        mids = [
            pltpu.VMEM((NCHUNK, *((3, 4) if o[1] < o[0] else (4, 3)), 4, RANKS, cols), BF16) for o in ORDERS
        ]
        return [pltpu.VMEM((NCHUNK, NPART, 7, 4, 4, RANKS, cols), BF16), *mids, pltpu.VMEM((NCHUNK, 4, 4, 4, RANKS, d_model), BF16)]

    n_sem = NCHUNK * NPART * 3
    dma = pltpu.SemaphoreType.DMA
    return pl.pallas_call(
        kernel,
        out_shape=jax.ShapeDtypeStruct(hidden.shape, hidden.dtype),
        in_specs=[pl.BlockSpec(memory_space=pl.ANY)] * 4,
        out_specs=pl.BlockSpec(memory_space=pltpu.VMEM),
        scratch_shapes=[
            pltpu.VMEM((tok, d_model), BF16),
            pltpu.VMEM((tok, n_exp), F32),
            pltpu.VMEM((d_model, ff), BF16),
            pltpu.VMEM((ff, d_model), BF16),
            *path(),
            *path(),
            pltpu.VMEM((2, 512, n_exp), BF16),
            pltpu.VMEM((NCHUNK, 3, half, 512), BF16),
            pltpu.VMEM((NCHUNK, 512, 1), F32),
            pltpu.VMEM((n_exp, n_exp), F32),
            pltpu.VMEM((7, 4, 4, 2, 1, n_exp), F32),
            pltpu.VMEM((3, 4, 4, 2, 1, n_exp), F32),
            pltpu.VMEM((2, 4, 4, 4, 1, n_exp), F32),
            pltpu.VMEM((2, half, n_exp), BF16),
            pltpu.VMEM((512, d_model), F32),
            pltpu.VMEM((2, half, d_model), F32),
            dma((4,)),
            dma((n_sem,)),
            dma((n_sem,)),
            dma((n_sem,)),
            dma((n_sem,)),
            dma((4,)),
            dma((4,)),
        ],
        compiler_params=pltpu.CompilerParams(collective_id=0, has_side_effects=True, vmem_limit_bytes=52 << 20),
    )(pltpu.with_memory_space_constraint(hidden, pltpu.HBM), pltpu.with_memory_space_constraint(logits, pltpu.HBM), w_in, w_out)


def solution(mesh):
    tok = P(("dp", "ep"), None)
    exp = P("ep", None, None)
    return jax.shard_map(layer, mesh=mesh, in_specs=(tok, tok, exp, exp), out_specs=tok, check_vma=False)
```

```python
import functools
import math

import jax
import jax.numpy as jnp
from jax import lax
from jax.experimental import pallas as pl
from jax.experimental.pallas import tpu as pltpu
from jax.sharding import PartitionSpec as P

MESH = pl.DeviceIdType.MESH
BF16, F32 = jnp.bfloat16, jnp.float32
NDEV = 128
RANKS = 8
KEEP = 512
ORDERS = ((2, 1, 0), (1, 0, 2), (0, 2, 1))
NPART = 3
NCHUNK = 4
FSTEPS = 3


def coords(d):
    return lax.div(d, 32), lax.rem(lax.div(d, 8), 4), lax.rem(lax.div(d, 2), 4), lax.rem(d, 2)


def shifted(me, offs, core):
    pos = coords(me)
    z, y, x = (lax.rem(p + (o + 4), 4) for p, o in zip(pos[:3], offs))
    return (z * 4 + y) * 8 + x * 2 + lax.rem(pos[3] + core, 2)


def along(dim, step):
    return tuple(step if d == dim else 0 for d in range(3))


def gelu(v):
    inner = v * (0.7978845608028654 + 0.035677408136300125 * (v * v))
    half = 0.5 * v
    return half + half * jnp.tanh(inner)


def split3(v):
    a = v.astype(BF16)
    r = v - a.astype(F32)
    b = r.astype(BF16)
    c = (r - b.astype(F32)).astype(BF16)
    return a, b, c


def dot(a, b):
    return jnp.dot(a, b, preferred_element_type=F32)


def dot_t(a, b):
    return lax.dot_general(a, b, (((1,), (1,)), ((), ())), preferred_element_type=F32)


class Exchange:
    def __init__(self, me, sign, hop, mids, final, send_sem, recv_sem, cols):
        self.me, self.sign, self.hop, self.mids, self.final = me, sign, hop, mids, final
        self.send_sem, self.recv_sem, self.cols = send_sem, recv_sem, cols
        self.peers = {}
        for core in range(2):
            for dim in range(3):
                for d in range(4):
                    self.peers[dim, d, core] = shifted(me, along(dim, sign * d), core)

    def sem(self, c, p, phase):
        return (c * NPART + p) * 3 + phase

    def copy(self, src, dst, c, p, phase, d, core):
        to = self.peers[ORDERS[p][phase], d, core]
        k = self.sem(c, p, phase)
        pltpu.make_async_remote_copy(
            src, dst, self.send_sem.at[k], self.recv_sem.at[k], device_id=(0, to), device_id_type=MESH
        ).start()

    def mid_at(self, p, c, d1):
        mid = self.mids[p]
        if ORDERS[p][1] < ORDERS[p][0]:
            return mid.at[c, d1 - 1]
        return mid.at[c, :, d1 - 1]

    def final_at(self, c, p, pick):
        idx = tuple(pick[ORDERS[p].index(d)] for d in range(3))
        return self.final.at[(c, *idx, slice(None), pl.ds(p * self.cols, self.cols))]

    def send0(self, c, p):
        for d in (2, 1, 3):
            self.copy(self.hop.at[c, p, d - 1], self.hop.at[c, p, 3 + d], c, p, 0, d, 0)

    def send1(self, c, p):
        for d in (2, 1, 3):
            self.copy(self.hop.at[c, p, pl.ds(3, 4), d], self.mid_at(p, c, d), c, p, 1, d, 0)

    def send2(self, c, p):
        core = c % 2
        for d in (2, 1, 3, 0):
            if d == 0 and core == 0:
                continue
            self.copy(self.hop.at[c, p, pl.ds(3, 4), 0, d], self.final_at(c, p, (pl.ds(0, 4), 0, d)), c, p, 2, d, core)
            self.copy(self.mids[p].at[c, :, :, d], self.final_at(c, p, (pl.ds(0, 4), pl.ds(1, 3), d)), c, p, 2, d, core)

    def own(self, c, p):
        self.final_set(c, p, (pl.ds(0, 4), 0, 0), self.hop[c, p, pl.ds(3, 4), 0, 0])
        self.final_set(c, p, (pl.ds(0, 4), pl.ds(1, 3), 0), self.mids[p][c, :, :, 0])

    def final_set(self, c, p, pick, value):
        idx = tuple(pick[ORDERS[p].index(d)] for d in range(3))
        self.final[(c, *idx, slice(None), pl.ds(p * self.cols, self.cols))] = value

    def region(self, c, p, phase):
        if phase == 0:
            return self.hop.at[c, p, pl.ds(4, 3)]
        if phase == 1:
            return self.mids[p].at[c]
        part = pl.ds(0, 4) if c % 2 else pl.ds(1, 3)
        return self.final_at(c, p, (pl.ds(0, 4), pl.ds(0, 4), part))

    def wait_recv(self, c, p, phase):
        r = self.region(c, p, phase)
        pltpu.make_async_copy(r, r, self.recv_sem.at[self.sem(c, p, phase)]).wait()

    def wait_send(self, c, p, phase):
        r = self.region(c, p, phase)
        pltpu.make_async_copy(r, r, self.send_sem.at[self.sem(c, p, phase)]).wait()

    def first(self, c):
        for p in range(NPART):
            self.send0(c, p)

    def second(self, c):
        for p in range(NPART):
            self.wait_recv(c, p, 0)
            self.send1(c, p)

    def third(self, c):
        for p in range(NPART):
            self.wait_recv(c, p, 1)
            self.send2(c, p)

    def arrived_part(self, c, p):
        self.wait_recv(c, p, 2)
        if c % 2 == 0:
            self.own(c, p)

    def arrived(self, c):
        for p in range(NPART):
            self.arrived_part(c, p)

    def drain(self, chunks, phases=(0, 1, 2)):
        for c in chunks:
            for p in range(NPART):
                for phase in phases:
                    self.wait_send(c, p, phase)


def kernel(
    x_hbm, l_hbm, win_hbm, wout_hbm, out_ref,
    x_ref, l_ref, win, wout, hop_i, mid_i0, mid_i1, mid_i2, fin_i, hop_r, mid_r0, mid_r1, mid_r2, fin_r,
    place, comb, mask, tops, tell_hop, tell_mid, told, rank, acc, yacc,
    load_sem, send_i, recv_i, send_r, recv_r, tell_send, tell_recv,
):
    me = lax.axis_index("ep")
    half, n_exp = l_ref.shape[0] // 2, l_ref.shape[1]
    d_model, ff = win.shape
    cols = d_model // NPART
    ftile = ff // FSTEPS
    rows = 64 * RANKS

    loads = [
        pltpu.make_async_copy(s, d, load_sem.at[i])
        for i, (s, d) in enumerate(((l_hbm, l_ref), (x_hbm, x_ref), (win_hbm.at[0], win), (wout_hbm.at[0], wout)))
    ]
    for ld in loads:
        ld.start()

    barrier = pltpu.get_barrier_semaphore()

    inward = Exchange(me, 1, hop_i, (mid_i0, mid_i1, mid_i2), fin_i, send_i, recv_i, cols)
    back = Exchange(me, -1, hop_r, (mid_r0, mid_r1, mid_r2), fin_r, send_r, recv_r, cols)

    peers = [inward.peers[dim, d, core] for core in range(2) for dim in range(3) for d in (1, 2, 3)] + [inward.peers[0, 0, 1]]
    for to in peers:
        pl.semaphore_signal(barrier, inc=1, device_id=(0, to), device_id_type=MESH)

    pos = coords(me)
    for core in range(2):
        q = lax.broadcasted_iota(jnp.int32, (rows, n_exp), 0)
        e = lax.broadcasted_iota(jnp.int32, (rows, n_exp), 1)
        ez = ((q >> 7) + pos[0]) & 3
        ey = ((q >> 5) + pos[1]) & 3
        ex = ((q >> 3) + pos[2]) & 3
        ec = (pos[3] + core) & 1
        want = ez * 32 + ey * 8 + ex * 2 + ec
        place[core] = jnp.where(e == want, 1.0, 0.0).astype(BF16)

    def put_blocks(dst, c, value):
        for z in range(4):
            for y in range(4):
                at = (z * 4 + y) * 32
                xs = value[at : at + 32, :].reshape(4, 8, d_model).astype(BF16)
                p0, p1, p2 = (xs[:, :, p * cols : (p + 1) * cols] for p in range(NPART))
                dst[c, 0, pl.ds(0, 3), y, z] = p0[1:]
                dst[c, 0, 3, y, z] = p0[0]
                dst[c, 1, (y + 3) % 4, z] = p1
                dst[c, 2, (z + 3) % 4, :, y] = p2

    def select(m):
        cur = l_ref[m * half : (m + 1) * half, :]
        rk = jnp.full(cur.shape, 15.0, F32)
        for r in range(RANKS):
            top = jnp.max(cur, axis=0, keepdims=True)
            hit = cur == top
            rk = jnp.where(hit, float(r), rk)
            cur = jnp.where(hit, -1e30, cur)
            for g in range(8):
                at = g * 16 + m * RANKS + r
                tops[at : at + 1, :] = top
        rank[m] = rk.astype(BF16)

    def gather(c):
        m, core = c // 2, c % 2
        wide = dot_t(place[core], rank[m])
        r_of = (lax.broadcasted_iota(jnp.int32, wide.shape, 0) & 7).astype(F32)
        pick = jnp.where(wide == r_of, 1.0, 0.0).astype(BF16)
        put_blocks(hop_i, c, dot(pick, x_ref[m * half : (m + 1) * half, :]))

    def tell_copy(src, dst, phase, dim, d, core):
        pltpu.make_async_remote_copy(
            src, dst, tell_send.at[phase], tell_recv.at[phase], device_id=(0, inward.peers[dim, d, core]), device_id_type=MESH
        ).start()

    def tell_wait(sem, phase, ref):
        pltpu.make_async_copy(ref, ref, sem.at[phase]).wait()

    def tell_first():
        q = lax.broadcasted_iota(jnp.int32, (NDEV, n_exp), 0)
        e = lax.broadcasted_iota(jnp.int32, (NDEV, n_exp), 1)
        ex = ((q >> 5) + 1 + pos[2]) & 3
        ey = ((q >> 3) + pos[1]) & 3
        ez = ((q >> 1) + pos[0]) & 3
        ec = (q + pos[3]) & 1
        at = jnp.where(e == ez * 32 + ey * 8 + ex * 2 + ec, 1.0, 0.0).astype(BF16)
        hi, mid, low = (dot_t(at, v) for v in split3(tops[...]))
        tell_hop[0:4] = ((hi + mid) + low).reshape(4, 4, 4, 2, 1, n_exp)
        for d in (2, 1, 3):
            tell_copy(tell_hop.at[d - 1], tell_hop.at[3 + d], 0, 2, d, 0)

    def tell_second():
        tell_wait(tell_recv, 0, tell_hop.at[pl.ds(4, 3)])
        for d in (2, 1, 3):
            tell_copy(tell_hop.at[pl.ds(3, 4), d], tell_mid.at[d - 1], 1, 1, d, 0)

    def tell_third():
        tell_wait(tell_recv, 1, tell_mid)
        for core in range(2):
            for d in (2, 1, 3, 0):
                if core or d:
                    tell_copy(tell_hop.at[pl.ds(3, 4), 0, d, core], told.at[core, d, 0], 3 - core, 0, d, core)
                    tell_copy(tell_mid.at[:, :, d, core], told.at[core, d, pl.ds(1, 3)], 3 - core, 0, d, core)

    def owner_cut():
        for ref, sem in ((told.at[1], tell_recv.at[2]), (told.at[0, pl.ds(1, 3)], tell_recv.at[3])):
            pltpu.make_async_copy(ref, ref, sem).wait()
        told[0, 0, 0] = tell_hop[3:7, 0, 0, 0]
        told[0, 0, 1:4] = tell_mid[:, :, 0, 0]
        seen = told[...].reshape(NDEV, n_exp)
        lane = lax.broadcasted_iota(jnp.int32, (n_exp, n_exp), 1)
        row = lax.broadcasted_iota(jnp.int32, (n_exp, n_exp), 0)
        same = jnp.where((lane >> 3) == (row >> 3), 1.0, 0.0).astype(BF16)
        first = jnp.where(((row & 7) == 0) & (((lane >> 3) & 1) == ((row >> 3) & 1)), 1.0, 0.0).astype(BF16)
        group = (lax.broadcasted_iota(jnp.int32, (8, n_exp), 1) >> 4).astype(F32)
        base = jnp.full((8, n_exp), -8.0, F32)
        width = 2.0
        for _ in range(8):
            cand = base + group * width
            over = jnp.where(seen >= cand[0:1], 1.0, 0.0)
            cnt = jnp.sum(over, axis=0, keepdims=True)
            cnt = dot(jnp.broadcast_to(cnt, (8, n_exp)).astype(BF16), same)
            flag = jnp.where(cnt >= float(KEEP), 1.0, 0.0).astype(BF16)
            base = base + (dot(flag, first) - 1.0) * width
            width = width / 8.0
        chosen = jnp.where(seen >= base[0:1], 1.0, 0.0).astype(BF16)
        for core in range(2):
            q = lax.broadcasted_iota(jnp.int32, (rows, NDEV), 0)
            src = lax.broadcasted_iota(jnp.int32, (rows, NDEV), 1)
            wide = dot(jnp.where(src == (q >> 3) + core * 64, 1.0, 0.0).astype(BF16), chosen)
            for m in range(2):
                keep = jnp.where(src == (q & 7) + m * 8, wide, 0.0)
                mask[m * 2 + core] = jnp.sum(keep, axis=1, keepdims=True)

    def gates():
        for m in range(2):
            lg = l_ref[m * half : (m + 1) * half, :]
            ex = jnp.exp(lg - jnp.max(lg, axis=1, keepdims=True))
            terms = split3(ex / jnp.sum(ex, axis=1, keepdims=True))
            for core in range(2):
                wide = dot_t(rank[m], place[core])
                r_of = (lax.broadcasted_iota(jnp.int32, wide.shape, 1) & 7).astype(F32)
                hit = wide == r_of
                for i, term in enumerate(terms):
                    comb[m * 2 + core, i] = jnp.where(hit, dot_t(term, place[core]), 0.0).astype(BF16)

    def drain_early():
        inward.drain(range(NCHUNK))
        tell_wait(tell_send, 0, tell_hop.at[pl.ds(4, 3)])
        tell_wait(tell_send, 1, tell_mid)
        for ref, sem in ((told.at[1], tell_send.at[2]), (told.at[0, pl.ds(1, 3)], tell_send.at[3])):
            pltpu.make_async_copy(ref, ref, sem).wait()

    def combine(c):
        m, core = c // 2, c % 2
        if c == 2:
            drain_early()
        if c == 3:
            back.drain(range(3))
            back.drain((3,), (0, 1))
        for p in range(NPART):
            back.arrived_part(c, p)
            at = slice(p * cols, (p + 1) * cols)
            y = fin_r[c, :, :, :, :, at].reshape(rows, cols)
            total = dot(comb[c, 0], y) + dot(comb[c, 1], y) + dot(comb[c, 2], y)
            if core == 0:
                yacc[m, :, at] = total
            else:
                both = x_ref[m * half : (m + 1) * half, at].astype(F32) + (yacc[m, :, at] + total)
                out_ref[m * half : (m + 1) * half, at] = both.astype(BF16)

    def more():
        gather(2)
        gather(3)

    loads[0].wait()
    tops[...] = jnp.zeros_like(tops)
    select(0)
    loads[1].wait()
    gather(0)
    pl.semaphore_wait(barrier, len(peers))
    inward.first(0)
    select(1)
    tell_first()
    gather(1)
    inward.first(1)
    more()
    inward.first(3)
    tell_second()
    inward.second(0)
    inward.first(2)
    inward.second(1)
    tell_third()
    inward.third(0)
    inward.second(2)
    inward.third(1)
    inward.second(3)
    owner_cut()
    loads[2].wait()
    loads[3].wait()

    during = {
        1: [lambda: inward.third(2)],
        4: [lambda: inward.third(3)],
        7: [lambda: back.second(0)],
        9: [lambda: back.second(1)],
    }

    def step(i, _):
        c, f = lax.div(i, FSTEPS), lax.rem(i, FSTEPS)
        for k in range(NCHUNK):
            @pl.when(i == k * FSTEPS)
            def _():
                inward.arrived(k)
                acc[...] = jnp.zeros_like(acc)

        at = pl.multiple_of(f * ftile, ftile)
        chunk = fin_i[c].reshape(rows, d_model)
        cut = rows // 2
        up = [dot(chunk[r : r + cut], win[:, pl.ds(at, ftile)]) for r in (0, cut)]
        for r, pre in zip((0, cut), up):
            acc[r : r + cut] += dot(gelu(pre).astype(BF16), wout[pl.ds(at, ftile), :])

        for k in range(NCHUNK):
            @pl.when(i == k * FSTEPS + FSTEPS - 1)
            def _():
                put_blocks(hop_r, k, jnp.where(mask[k] > 0.5, acc[...], 0.0))
                back.first(k)
        for at_i, todo in during.items():
            @pl.when(i == at_i)
            def _():
                for fn in todo:
                    fn()
        return 0

    lax.fori_loop(0, NCHUNK * FSTEPS, step, 0)

    back.third(0)
    back.second(2)
    gates()
    back.second(3)
    back.third(1)
    combine(0)
    back.third(2)
    back.third(3)
    combine(1)
    combine(2)
    combine(3)

    back.drain((3,), (2,))


def layer(hidden, logits, w_in, w_out):
    tok, d_model = hidden.shape
    n_exp = logits.shape[1]
    ff = w_in.shape[2]
    cols = d_model // NPART
    half = tok // 2

    def path():
        mids = [
            pltpu.VMEM((NCHUNK, *((3, 4) if o[1] < o[0] else (4, 3)), 4, RANKS, cols), BF16) for o in ORDERS
        ]
        return [pltpu.VMEM((NCHUNK, NPART, 7, 4, 4, RANKS, cols), BF16), *mids, pltpu.VMEM((NCHUNK, 4, 4, 4, RANKS, d_model), BF16)]

    n_sem = NCHUNK * NPART * 3
    dma = pltpu.SemaphoreType.DMA
    return pl.pallas_call(
        kernel,
        out_shape=jax.ShapeDtypeStruct(hidden.shape, hidden.dtype),
        in_specs=[pl.BlockSpec(memory_space=pl.ANY)] * 4,
        out_specs=pl.BlockSpec(memory_space=pltpu.VMEM),
        scratch_shapes=[
            pltpu.VMEM((tok, d_model), BF16),
            pltpu.VMEM((tok, n_exp), F32),
            pltpu.VMEM((d_model, ff), BF16),
            pltpu.VMEM((ff, d_model), BF16),
            *path(),
            *path(),
            pltpu.VMEM((2, 512, n_exp), BF16),
            pltpu.VMEM((NCHUNK, 3, half, 512), BF16),
            pltpu.VMEM((NCHUNK, 512, 1), F32),
            pltpu.VMEM((n_exp, n_exp), F32),
            pltpu.VMEM((7, 4, 4, 2, 1, n_exp), F32),
            pltpu.VMEM((3, 4, 4, 2, 1, n_exp), F32),
            pltpu.VMEM((2, 4, 4, 4, 1, n_exp), F32),
            pltpu.VMEM((2, half, n_exp), BF16),
            pltpu.VMEM((512, d_model), F32),
            pltpu.VMEM((2, half, d_model), F32),
            dma((4,)),
            dma((n_sem,)),
            dma((n_sem,)),
            dma((n_sem,)),
            dma((n_sem,)),
            dma((4,)),
            dma((4,)),
        ],
        compiler_params=pltpu.CompilerParams(collective_id=0, has_side_effects=True, vmem_limit_bytes=52 << 20),
    )(pltpu.with_memory_space_constraint(hidden, pltpu.HBM), pltpu.with_memory_space_constraint(logits, pltpu.HBM), w_in, w_out)


def solution(mesh):
    tok = P(("dp", "ep"), None)
    exp = P("ep", None, None)
    return jax.shard_map(layer, mesh=mesh, in_specs=(tok, tok, exp, exp), out_specs=tok, check_vma=False)
```

```python
import functools
import math

import jax
import jax.numpy as jnp
from jax import lax
from jax.experimental import pallas as pl
from jax.experimental.pallas import tpu as pltpu
from jax.sharding import PartitionSpec as P

MESH = pl.DeviceIdType.MESH
BF16, F32 = jnp.bfloat16, jnp.float32
NDEV = 128
RANKS = 8
KEEP = 512
ORDERS = ((2, 1, 0), (1, 0, 2), (0, 2, 1))
NPART = 3
NCHUNK = 4
FSTEPS = 3


def coords(d):
    return lax.div(d, 32), lax.rem(lax.div(d, 8), 4), lax.rem(lax.div(d, 2), 4), lax.rem(d, 2)


def shifted(me, offs, core):
    pos = coords(me)
    z, y, x = (lax.rem(p + (o + 4), 4) for p, o in zip(pos[:3], offs))
    return (z * 4 + y) * 8 + x * 2 + lax.rem(pos[3] + core, 2)


def along(dim, step):
    return tuple(step if d == dim else 0 for d in range(3))


def gelu(v):
    inner = v * (0.7978845608028654 + 0.035677408136300125 * (v * v))
    half = 0.5 * v
    return half + half * jnp.tanh(inner)


def split3(v):
    a = v.astype(BF16)
    r = v - a.astype(F32)
    b = r.astype(BF16)
    c = (r - b.astype(F32)).astype(BF16)
    return a, b, c


def dot(a, b):
    return jnp.dot(a, b, preferred_element_type=F32)


def dot_t(a, b):
    return lax.dot_general(a, b, (((1,), (1,)), ((), ())), preferred_element_type=F32)


class Exchange:
    def __init__(self, me, sign, hop, mids, final, send_sem, recv_sem, cols):
        self.me, self.sign, self.hop, self.mids, self.final = me, sign, hop, mids, final
        self.send_sem, self.recv_sem, self.cols = send_sem, recv_sem, cols
        self.peers = {}
        for core in range(2):
            for dim in range(3):
                for d in range(4):
                    self.peers[dim, d, core] = shifted(me, along(dim, sign * d), core)

    def sem(self, c, p, phase):
        return (c * NPART + p) * 3 + phase

    def copy(self, src, dst, c, p, phase, d, core):
        to = self.peers[ORDERS[p][phase], d, core]
        k = self.sem(c, p, phase)
        pltpu.make_async_remote_copy(
            src, dst, self.send_sem.at[k], self.recv_sem.at[k], device_id=(0, to), device_id_type=MESH
        ).start()

    def mid_at(self, p, c, d1):
        mid = self.mids[p]
        if ORDERS[p][1] < ORDERS[p][0]:
            return mid.at[c, d1 - 1]
        return mid.at[c, :, d1 - 1]

    def final_at(self, c, p, pick):
        idx = tuple(pick[ORDERS[p].index(d)] for d in range(3))
        return self.final.at[(c, *idx, slice(None), pl.ds(p * self.cols, self.cols))]

    def send0(self, c, p):
        for d in (2, 1, 3):
            self.copy(self.hop.at[c, p, d - 1], self.hop.at[c, p, 3 + d], c, p, 0, d, 0)

    def send1(self, c, p):
        for d in (2, 1, 3):
            self.copy(self.hop.at[c, p, pl.ds(3, 4), d], self.mid_at(p, c, d), c, p, 1, d, 0)

    def send2(self, c, p):
        core = c % 2
        for d in (2, 1, 3, 0):
            if d == 0 and core == 0:
                continue
            self.copy(self.hop.at[c, p, pl.ds(3, 4), 0, d], self.final_at(c, p, (pl.ds(0, 4), 0, d)), c, p, 2, d, core)
            self.copy(self.mids[p].at[c, :, :, d], self.final_at(c, p, (pl.ds(0, 4), pl.ds(1, 3), d)), c, p, 2, d, core)

    def own(self, c, p):
        self.final_set(c, p, (pl.ds(0, 4), 0, 0), self.hop[c, p, pl.ds(3, 4), 0, 0])
        self.final_set(c, p, (pl.ds(0, 4), pl.ds(1, 3), 0), self.mids[p][c, :, :, 0])

    def final_set(self, c, p, pick, value):
        idx = tuple(pick[ORDERS[p].index(d)] for d in range(3))
        self.final[(c, *idx, slice(None), pl.ds(p * self.cols, self.cols))] = value

    def region(self, c, p, phase):
        if phase == 0:
            return self.hop.at[c, p, pl.ds(4, 3)]
        if phase == 1:
            return self.mids[p].at[c]
        part = pl.ds(0, 4) if c % 2 else pl.ds(1, 3)
        return self.final_at(c, p, (pl.ds(0, 4), pl.ds(0, 4), part))

    def wait_recv(self, c, p, phase):
        r = self.region(c, p, phase)
        pltpu.make_async_copy(r, r, self.recv_sem.at[self.sem(c, p, phase)]).wait()

    def wait_send(self, c, p, phase):
        r = self.region(c, p, phase)
        pltpu.make_async_copy(r, r, self.send_sem.at[self.sem(c, p, phase)]).wait()

    def first(self, c):
        for p in range(NPART):
            self.send0(c, p)

    def second(self, c):
        for p in range(NPART):
            self.wait_recv(c, p, 0)
            self.send1(c, p)

    def third(self, c):
        for p in range(NPART):
            self.wait_recv(c, p, 1)
            self.send2(c, p)

    def arrived_part(self, c, p):
        self.wait_recv(c, p, 2)
        if c % 2 == 0:
            self.own(c, p)

    def arrived(self, c):
        for p in range(NPART):
            self.arrived_part(c, p)

    def drain(self, chunks, phases=(0, 1, 2)):
        for c in chunks:
            for p in range(NPART):
                for phase in phases:
                    self.wait_send(c, p, phase)


def kernel(
    x_hbm, l_hbm, win_hbm, wout_hbm, out_ref,
    x_ref, l_ref, win, wout, hop_i, mid_i0, mid_i1, mid_i2, fin_i, hop_r, mid_r0, mid_r1, mid_r2, fin_r,
    place, comb, mask, tops, tell_hop, tell_mid, told, rank, acc, yacc,
    load_sem, send_i, recv_i, send_r, recv_r, tell_send, tell_recv,
):
    me = lax.axis_index("ep")
    half, n_exp = l_ref.shape[0] // 2, l_ref.shape[1]
    d_model, ff = win.shape
    cols = d_model // NPART
    ftile = ff // FSTEPS
    rows = 64 * RANKS

    loads = [
        pltpu.make_async_copy(s, d, load_sem.at[i])
        for i, (s, d) in enumerate(((l_hbm, l_ref), (x_hbm, x_ref), (win_hbm.at[0], win), (wout_hbm.at[0], wout)))
    ]
    for ld in loads:
        ld.start()

    barrier = pltpu.get_barrier_semaphore()

    inward = Exchange(me, 1, hop_i, (mid_i0, mid_i1, mid_i2), fin_i, send_i, recv_i, cols)
    back = Exchange(me, -1, hop_r, (mid_r0, mid_r1, mid_r2), fin_r, send_r, recv_r, cols)

    peers = [inward.peers[dim, d, core] for core in range(2) for dim in range(3) for d in (1, 2, 3)] + [inward.peers[0, 0, 1]]
    for to in peers:
        pl.semaphore_signal(barrier, inc=1, device_id=(0, to), device_id_type=MESH)

    pos = coords(me)
    for core in range(2):
        q = lax.broadcasted_iota(jnp.int32, (rows, n_exp), 0)
        e = lax.broadcasted_iota(jnp.int32, (rows, n_exp), 1)
        ez = ((q >> 7) + pos[0]) & 3
        ey = ((q >> 5) + pos[1]) & 3
        ex = ((q >> 3) + pos[2]) & 3
        ec = (pos[3] + core) & 1
        want = ez * 32 + ey * 8 + ex * 2 + ec
        place[core] = jnp.where(e == want, 1.0, 0.0).astype(BF16)

    def put_blocks(dst, c, value):
        for z in range(4):
            for y in range(4):
                at = (z * 4 + y) * 32
                xs = value[at : at + 32, :].reshape(4, 8, d_model).astype(BF16)
                p0, p1, p2 = (xs[:, :, p * cols : (p + 1) * cols] for p in range(NPART))
                dst[c, 0, pl.ds(0, 3), y, z] = p0[1:]
                dst[c, 0, 3, y, z] = p0[0]
                dst[c, 1, (y + 3) % 4, z] = p1
                dst[c, 2, (z + 3) % 4, :, y] = p2

    def select(m):
        cur = l_ref[m * half : (m + 1) * half, :]
        rk = jnp.full(cur.shape, 15.0, F32)
        for r in range(RANKS):
            top = jnp.max(cur, axis=0, keepdims=True)
            hit = cur == top
            rk = jnp.where(hit, float(r), rk)
            cur = jnp.where(hit, -1e30, cur)
            for g in range(8):
                at = g * 16 + m * RANKS + r
                tops[at : at + 1, :] = top
        rank[m] = rk.astype(BF16)

    def gather(c):
        m, core = c // 2, c % 2
        wide = dot_t(place[core], rank[m])
        r_of = (lax.broadcasted_iota(jnp.int32, wide.shape, 0) & 7).astype(F32)
        pick = jnp.where(wide == r_of, 1.0, 0.0).astype(BF16)
        put_blocks(hop_i, c, dot(pick, x_ref[m * half : (m + 1) * half, :]))

    def tell_copy(src, dst, phase, dim, d, core):
        pltpu.make_async_remote_copy(
            src, dst, tell_send.at[phase], tell_recv.at[phase], device_id=(0, inward.peers[dim, d, core]), device_id_type=MESH
        ).start()

    def tell_wait(sem, phase, ref):
        pltpu.make_async_copy(ref, ref, sem.at[phase]).wait()

    def tell_first():
        q = lax.broadcasted_iota(jnp.int32, (NDEV, n_exp), 0)
        e = lax.broadcasted_iota(jnp.int32, (NDEV, n_exp), 1)
        ex = ((q >> 5) + 1 + pos[2]) & 3
        ey = ((q >> 3) + pos[1]) & 3
        ez = ((q >> 1) + pos[0]) & 3
        ec = (q + pos[3]) & 1
        at = jnp.where(e == ez * 32 + ey * 8 + ex * 2 + ec, 1.0, 0.0).astype(BF16)
        hi, mid, low = (dot_t(at, v) for v in split3(tops[...]))
        tell_hop[0:4] = ((hi + mid) + low).reshape(4, 4, 4, 2, 1, n_exp)
        for d in (2, 1, 3):
            tell_copy(tell_hop.at[d - 1], tell_hop.at[3 + d], 0, 2, d, 0)

    def tell_second():
        tell_wait(tell_recv, 0, tell_hop.at[pl.ds(4, 3)])
        for d in (2, 1, 3):
            tell_copy(tell_hop.at[pl.ds(3, 4), d], tell_mid.at[d - 1], 1, 1, d, 0)

    def tell_third():
        tell_wait(tell_recv, 1, tell_mid)
        for core in range(2):
            for d in (2, 1, 3, 0):
                if core or d:
                    tell_copy(tell_hop.at[pl.ds(3, 4), 0, d, core], told.at[core, d, 0], 3 - core, 0, d, core)
                    tell_copy(tell_mid.at[:, :, d, core], told.at[core, d, pl.ds(1, 3)], 3 - core, 0, d, core)

    def owner_cut():
        for ref, sem in ((told.at[1], tell_recv.at[2]), (told.at[0, pl.ds(1, 3)], tell_recv.at[3])):
            pltpu.make_async_copy(ref, ref, sem).wait()
        told[0, 0, 0] = tell_hop[3:7, 0, 0, 0]
        told[0, 0, 1:4] = tell_mid[:, :, 0, 0]
        seen = told[...].reshape(NDEV, n_exp)
        lane = lax.broadcasted_iota(jnp.int32, (n_exp, n_exp), 1)
        row = lax.broadcasted_iota(jnp.int32, (n_exp, n_exp), 0)
        same = jnp.where((lane >> 3) == (row >> 3), 1.0, 0.0).astype(BF16)
        first = jnp.where(((row & 7) == 0) & (((lane >> 3) & 1) == ((row >> 3) & 1)), 1.0, 0.0).astype(BF16)
        group = (lax.broadcasted_iota(jnp.int32, (8, n_exp), 1) >> 4).astype(F32)
        base = jnp.full((8, n_exp), -8.0, F32)
        width = 2.0
        for _ in range(8):
            cand = base + group * width
            over = jnp.where(seen >= cand[0:1], 1.0, 0.0)
            cnt = jnp.sum(over, axis=0, keepdims=True)
            cnt = dot(jnp.broadcast_to(cnt, (8, n_exp)).astype(BF16), same)
            flag = jnp.where(cnt >= float(KEEP), 1.0, 0.0).astype(BF16)
            base = base + (dot(flag, first) - 1.0) * width
            width = width / 8.0
        chosen = jnp.where(seen >= base[0:1], 1.0, 0.0).astype(BF16)
        for core in range(2):
            q = lax.broadcasted_iota(jnp.int32, (rows, NDEV), 0)
            src = lax.broadcasted_iota(jnp.int32, (rows, NDEV), 1)
            wide = dot(jnp.where(src == (q >> 3) + core * 64, 1.0, 0.0).astype(BF16), chosen)
            for m in range(2):
                keep = jnp.where(src == (q & 7) + m * 8, wide, 0.0)
                mask[m * 2 + core] = jnp.sum(keep, axis=1, keepdims=True)

    def gates():
        for m in range(2):
            lg = l_ref[m * half : (m + 1) * half, :]
            ex = jnp.exp(lg - jnp.max(lg, axis=1, keepdims=True))
            terms = split3(ex / jnp.sum(ex, axis=1, keepdims=True))
            for core in range(2):
                wide = dot_t(rank[m], place[core])
                r_of = (lax.broadcasted_iota(jnp.int32, wide.shape, 1) & 7).astype(F32)
                hit = wide == r_of
                for i, term in enumerate(terms):
                    comb[m * 2 + core, i] = jnp.where(hit, dot_t(term, place[core]), 0.0).astype(BF16)

    def drain_early():
        inward.drain(range(NCHUNK))
        tell_wait(tell_send, 0, tell_hop.at[pl.ds(4, 3)])
        tell_wait(tell_send, 1, tell_mid)
        for ref, sem in ((told.at[1], tell_send.at[2]), (told.at[0, pl.ds(1, 3)], tell_send.at[3])):
            pltpu.make_async_copy(ref, ref, sem).wait()

    def combine(c):
        m, core = c // 2, c % 2
        if c == 2:
            drain_early()
        if c == 3:
            back.drain(range(3))
            back.drain((3,), (0, 1))
        for p in range(NPART):
            back.arrived_part(c, p)
            at = slice(p * cols, (p + 1) * cols)
            y = fin_r[c, :, :, :, :, at].reshape(rows, cols)
            total = dot(comb[c, 0], y) + dot(comb[c, 1], y) + dot(comb[c, 2], y)
            if core == 0:
                yacc[m, :, at] = total
            else:
                both = x_ref[m * half : (m + 1) * half, at].astype(F32) + (yacc[m, :, at] + total)
                out_ref[m * half : (m + 1) * half, at] = both.astype(BF16)

    def more():
        gather(2)
        gather(3)

    loads[0].wait()
    tops[...] = jnp.zeros_like(tops)
    select(0)
    loads[1].wait()
    gather(0)
    pl.semaphore_wait(barrier, len(peers))
    inward.first(0)
    select(1)
    tell_first()
    gather(1)
    inward.first(1)
    more()
    inward.first(3)
    tell_second()
    inward.second(0)
    inward.first(2)
    inward.second(1)
    tell_third()
    inward.third(0)
    inward.second(2)
    inward.third(1)
    inward.second(3)
    owner_cut()
    loads[2].wait()
    loads[3].wait()

    during = {
        1: [lambda: inward.third(2)],
        4: [lambda: inward.third(3)],
        7: [lambda: back.second(0)],
        10: [lambda: back.second(1)],
    }

    def step(i, _):
        c, f = lax.div(i, FSTEPS), lax.rem(i, FSTEPS)
        for k in range(NCHUNK):
            @pl.when(i == k * FSTEPS)
            def _():
                inward.arrived(k)
                acc[...] = jnp.zeros_like(acc)

        at = pl.multiple_of(f * ftile, ftile)
        chunk = fin_i[c].reshape(rows, d_model)
        cut = rows // 2
        up = [dot(chunk[r : r + cut], win[:, pl.ds(at, ftile)]) for r in (0, cut)]
        for r, pre in zip((0, cut), up):
            acc[r : r + cut] += dot(gelu(pre).astype(BF16), wout[pl.ds(at, ftile), :])

        for k in range(NCHUNK):
            @pl.when(i == k * FSTEPS + FSTEPS - 1)
            def _():
                put_blocks(hop_r, k, jnp.where(mask[k] > 0.5, acc[...], 0.0))
                back.first(k)
        for at_i, todo in during.items():
            @pl.when(i == at_i)
            def _():
                for fn in todo:
                    fn()
        return 0

    lax.fori_loop(0, NCHUNK * FSTEPS, step, 0)

    back.third(0)
    back.second(2)
    gates()
    back.second(3)
    back.third(1)
    combine(0)
    back.third(2)
    back.third(3)
    combine(1)
    combine(2)
    combine(3)

    back.drain((3,), (2,))


def layer(hidden, logits, w_in, w_out):
    tok, d_model = hidden.shape
    n_exp = logits.shape[1]
    ff = w_in.shape[2]
    cols = d_model // NPART
    half = tok // 2

    def path():
        mids = [
            pltpu.VMEM((NCHUNK, *((3, 4) if o[1] < o[0] else (4, 3)), 4, RANKS, cols), BF16) for o in ORDERS
        ]
        return [pltpu.VMEM((NCHUNK, NPART, 7, 4, 4, RANKS, cols), BF16), *mids, pltpu.VMEM((NCHUNK, 4, 4, 4, RANKS, d_model), BF16)]

    n_sem = NCHUNK * NPART * 3
    dma = pltpu.SemaphoreType.DMA
    return pl.pallas_call(
        kernel,
        out_shape=jax.ShapeDtypeStruct(hidden.shape, hidden.dtype),
        in_specs=[pl.BlockSpec(memory_space=pl.ANY)] * 4,
        out_specs=pl.BlockSpec(memory_space=pltpu.VMEM),
        scratch_shapes=[
            pltpu.VMEM((tok, d_model), BF16),
            pltpu.VMEM((tok, n_exp), F32),
            pltpu.VMEM((d_model, ff), BF16),
            pltpu.VMEM((ff, d_model), BF16),
            *path(),
            *path(),
            pltpu.VMEM((2, 512, n_exp), BF16),
            pltpu.VMEM((NCHUNK, 3, half, 512), BF16),
            pltpu.VMEM((NCHUNK, 512, 1), F32),
            pltpu.VMEM((n_exp, n_exp), F32),
            pltpu.VMEM((7, 4, 4, 2, 1, n_exp), F32),
            pltpu.VMEM((3, 4, 4, 2, 1, n_exp), F32),
            pltpu.VMEM((2, 4, 4, 4, 1, n_exp), F32),
            pltpu.VMEM((2, half, n_exp), BF16),
            pltpu.VMEM((512, d_model), F32),
            pltpu.VMEM((2, half, d_model), F32),
            dma((4,)),
            dma((n_sem,)),
            dma((n_sem,)),
            dma((n_sem,)),
            dma((n_sem,)),
            dma((4,)),
            dma((4,)),
        ],
        compiler_params=pltpu.CompilerParams(collective_id=0, has_side_effects=True, vmem_limit_bytes=52 << 20),
    )(pltpu.with_memory_space_constraint(hidden, pltpu.HBM), pltpu.with_memory_space_constraint(logits, pltpu.HBM), w_in, w_out)


def solution(mesh):
    tok = P(("dp", "ep"), None)
    exp = P("ep", None, None)
    return jax.shard_map(layer, mesh=mesh, in_specs=(tok, tok, exp, exp), out_specs=tok, check_vma=False)
```
